128 devices in a mesh: graph: 1, nodes: 128 (over z, y, x, core).
Axes of the slice: x: 4, y: 4, z: 4, core: 2. Of those that a mesh axis runs over, the one named last changes fastest.
Arguments:
- node_feats: bfloat16 [131072, 300], P(('graph', 'nodes'))
- a_int: bfloat16 [131072, 1024], P(('graph', 'nodes'))
- a_halo: bfloat16 [131072, 512], P(('graph', 'nodes'))
- send_idx: int32 [512, 128], P(('graph', 'nodes'))
- w_first: bfloat16 [300, 512], replicated
- w_second: bfloat16 [512, 100], replicated
- grad_out: bfloat16 [131072, 100], P(('graph', 'nodes'))
Outputs:
- output 1: float32 [300, 512], P('graph')
- output 2: float32 [512, 100], P('graph')
- output 3: float32 [131072, 300], P(('graph', 'nodes'))
All inputs are finite; a program needn't handle non-finite values.
Results may differ from the reference program's by a relative error of at most 0.00627.
Values are sent between devices in bfloat16 or wider.
A program may use at most 1 GiB of HBM per device.

```python
import jax
import jax.numpy as jnp
from jax import lax

GROUP_SIZE = 128
NODES_DEV = 1024
HALO_SLOTS = 128
MAX_HOPS = 2
FEAT_IN = 300
HIDDEN = 512
CLASSES = 100
INNER_DEGREE = 16
HALO_DEGREE = 4

NUM_LINKS = 2 * MAX_HOPS
OFFSETS = [(link // 2 + 1) * (1 - 2 * (link % 2)) for link in range(NUM_LINKS)]


def draw_graph(key):
    key_count, key_order, key_blocks = jax.random.split(key, 3)
    window = 2 * HALO_SLOTS
    counts = jax.random.randint(key_count, (GROUP_SIZE, NUM_LINKS), HALO_SLOTS // 4, HALO_SLOTS + 1)
    counts = counts.at[0, 0].set(HALO_SLOTS)
    scores = jax.random.randint(key_order, (GROUP_SIZE, NUM_LINKS, window), 0, 65536) * window + jnp.arange(window)
    slot_order = jnp.argsort(scores, axis=-1)[:, :, :HALO_SLOTS]
    upward = jnp.array([offset > 0 for offset in OFFSETS])
    window_base = jnp.where(upward, NODES_DEV - window, 0)
    slot_pos = jnp.arange(HALO_SLOTS)
    used_slot = slot_pos[None, None, :] < counts[:, :, None]
    send_idx = jnp.where(used_slot, slot_order + window_base[None, :, None], 0).astype(jnp.int32)
    recv_counts = jnp.stack([jnp.roll(counts[:, link], OFFSETS[link]) for link in range(NUM_LINKS)], axis=1)
    row_pos = jnp.arange(NODES_DEV)
    low_half = row_pos < NODES_DEV // 2
    row_ok = jnp.where(upward[None, :], low_half[:, None], jnp.logical_not(low_half)[:, None])

    def one_device(inputs):
        dev_key, recv_count = inputs
        key_mask, key_inner, key_hmask, key_halo = jax.random.split(dev_key, 4)
        inner_mask = jnp.logical_or(jax.random.randint(key_mask, (NODES_DEV, NODES_DEV), 0, NODES_DEV) < INNER_DEGREE, row_pos[:, None] == row_pos[None, :])
        col_ok = slot_pos[None, :] < recv_count[:, None]
        halo_mask = (jax.random.randint(key_hmask, (NODES_DEV, NUM_LINKS, HALO_SLOTS), 0, HALO_SLOTS) < HALO_DEGREE) & row_ok[:, :, None] & col_ok[None, :, :]
        inner_w = jnp.where(inner_mask, jax.random.uniform(key_inner, (NODES_DEV, NODES_DEV), jnp.float32, 0.5, 1.5), 0.0)
        halo_w = jnp.where(halo_mask, jax.random.uniform(key_halo, (NODES_DEV, NUM_LINKS, HALO_SLOTS), jnp.float32, 0.5, 1.5), 0.0)
        degree = jnp.sum(inner_mask, axis=1) + jnp.sum(halo_mask, axis=(1, 2))
        row_scale = lax.rsqrt(degree.astype(jnp.float32))
        inner_adj = (inner_w * row_scale[:, None]).astype(jnp.bfloat16)
        halo_adj = (halo_w * row_scale[:, None, None]).reshape(NODES_DEV, NUM_LINKS * HALO_SLOTS).astype(jnp.bfloat16)
        return inner_adj, halo_adj

    inner_adj, halo_adj = lax.map(one_device, (jax.random.split(key_blocks, GROUP_SIZE), recv_counts))
    return (inner_adj.reshape(GROUP_SIZE * NODES_DEV, NODES_DEV), halo_adj.reshape(GROUP_SIZE * NODES_DEV, NUM_LINKS * HALO_SLOTS), send_idx.reshape(GROUP_SIZE * NUM_LINKS, HALO_SLOTS))


def setup_inputs(seed: int = 0, part: int = 0) -> dict:
    root_key = jax.random.key(seed)
    shared_key, parts_key = jax.random.split(root_key)
    key_first, key_second = jax.random.split(shared_key)
    part_key = jax.random.fold_in(parts_key, part)
    key_feats, key_grad, key_graph = jax.random.split(part_key, 3)
    rows_total = GROUP_SIZE * NODES_DEV
    node_feats = jax.random.normal(key_feats, (rows_total, FEAT_IN), jnp.float32).astype(jnp.bfloat16)
    grad_out = jax.random.normal(key_grad, (rows_total, CLASSES), jnp.float32).astype(jnp.bfloat16)
    w_first = (jax.random.normal(key_first, (FEAT_IN, HIDDEN), jnp.float32) * FEAT_IN ** -0.5).astype(jnp.bfloat16)
    w_second = (jax.random.normal(key_second, (HIDDEN, CLASSES), jnp.float32) * HIDDEN ** -0.5).astype(jnp.bfloat16)
    a_int, a_halo, send_idx = draw_graph(key_graph)
    return {"node_feats": node_feats, "a_int": a_int, "a_halo": a_halo, "send_idx": send_idx, "w_first": w_first, "w_second": w_second, "grad_out": grad_out}


def aggregate(a_int, a_halo, features, send_idx):
    feat_width = features.shape[-1]
    local_rows = features.reshape(GROUP_SIZE, NODES_DEV, feat_width)
    send_plan = send_idx.reshape(GROUP_SIZE, NUM_LINKS * HALO_SLOTS)
    sent_rows = jax.vmap(lambda rows_dev, plan_dev: jnp.take(rows_dev, plan_dev, axis=0))(local_rows, send_plan)
    sent_rows = sent_rows.reshape(GROUP_SIZE, NUM_LINKS, HALO_SLOTS, feat_width)
    halo_rows = jnp.stack([jnp.roll(sent_rows[:, link], OFFSETS[link], axis=0) for link in range(NUM_LINKS)], axis=1)
    halo_rows = halo_rows.reshape(GROUP_SIZE, NUM_LINKS * HALO_SLOTS, feat_width)
    blocks = (a_int.reshape(GROUP_SIZE, NODES_DEV, NODES_DEV), a_halo.reshape(GROUP_SIZE, NODES_DEV, NUM_LINKS * HALO_SLOTS), local_rows, halo_rows)

    def one_device(block):
        inner_adj, halo_adj, own_rows, remote_rows = block
        return jnp.dot(inner_adj, own_rows, preferred_element_type=jnp.float32) + jnp.dot(halo_adj, remote_rows, preferred_element_type=jnp.float32)

    return lax.map(one_device, blocks).reshape(GROUP_SIZE * NODES_DEV, feat_width)


def aggregate_back(a_int, a_halo, grad_rows, send_idx):
    feat_width = grad_rows.shape[-1]
    local_rows = grad_rows.reshape(GROUP_SIZE, NODES_DEV, feat_width)
    blocks = (a_int.reshape(GROUP_SIZE, NODES_DEV, NODES_DEV), a_halo.reshape(GROUP_SIZE, NODES_DEV, NUM_LINKS * HALO_SLOTS), local_rows)

    def one_device(block):
        inner_adj, halo_adj, own_rows = block
        inner_sum = jnp.dot(inner_adj.T, own_rows, preferred_element_type=jnp.float32)
        outward = jnp.dot(halo_adj.T, own_rows, preferred_element_type=jnp.float32).astype(jnp.bfloat16)
        return inner_sum, outward

    inner_sum, outward = lax.map(one_device, blocks)
    outward = outward.reshape(GROUP_SIZE, NUM_LINKS, HALO_SLOTS, feat_width)
    returned = jnp.stack([jnp.roll(outward[:, link], -OFFSETS[link], axis=0) for link in range(NUM_LINKS)], axis=1)
    returned = returned.reshape(GROUP_SIZE, NUM_LINKS * HALO_SLOTS, feat_width)
    send_plan = send_idx.reshape(GROUP_SIZE, NUM_LINKS * HALO_SLOTS)
    total_sum = jax.vmap(lambda sums_dev, plan_dev, rows_dev: sums_dev.at[plan_dev].add(rows_dev.astype(jnp.float32)))(inner_sum, send_plan, returned)
    return total_sum.reshape(GROUP_SIZE * NODES_DEV, feat_width)


def reference(node_feats, a_int, a_halo, send_idx, w_first, w_second, grad_out):
    z_first = aggregate(a_int, a_halo, node_feats, send_idx).astype(jnp.bfloat16)
    hidden = jnp.maximum(jnp.dot(z_first, w_first, preferred_element_type=jnp.float32), 0.0).astype(jnp.bfloat16)
    z_second = aggregate(a_int, a_halo, hidden, send_idx).astype(jnp.bfloat16)
    dw_second = jnp.dot(z_second.T, grad_out, preferred_element_type=jnp.float32)
    dz_second = jnp.dot(grad_out, w_second.T, preferred_element_type=jnp.float32).astype(jnp.bfloat16)
    d_hidden = aggregate_back(a_int, a_halo, dz_second, send_idx)
    grad_pre = jnp.where(hidden > 0, d_hidden, 0.0).astype(jnp.bfloat16)
    dw_first = jnp.dot(z_first.T, grad_pre, preferred_element_type=jnp.float32)
    dz_first = jnp.dot(grad_pre, w_first.T, preferred_element_type=jnp.float32).astype(jnp.bfloat16)
    grad_feats = aggregate_back(a_int, a_halo, dz_first, send_idx)
    return (dw_first, dw_second, grad_feats)
```

```python
import jax
import jax.numpy as jnp
from jax import lax
from jax.experimental import pallas as pl
from jax.experimental.pallas import tpu as pltpu
from jax.sharding import PartitionSpec as P

F32 = jnp.float32
BF16 = jnp.bfloat16
NX, NY, NZ = 4, 4, 4
PLANE = NY * NZ
OFFSETS = (1, -1, 2, -2)
LINKS = 4


def dot(a, b, ca, cb):
    return lax.dot_general(a, b, (((ca,), (cb,)), ((), ())), preferred_element_type=F32)


def build(n_dev, nodes, feat, hid, cls, slots):
    all_slots = LINKS * slots
    slab1 = (feat + 7) // 8 * 8
    slab2 = (cls + 7) // 8 * 8
    n_slab = hid // 128
    half_slabs = n_slab // 2
    used = half_slabs * (slab1 + slab2)
    chunk = -(-used // (PLANE * 8)) * 8
    half = chunk * PLANE
    off2 = half_slabs * slab1

    def kernel(h0_hbm, aint_hbm, ahalo_hbm, idx_hbm, w0_hbm, w1_hbm, g_hbm,
               dw1_out, dw2_out, gf_hbm,
               h0, aint, ahalo, idx, w0, w1, g,
               pt, e1, z0, ft, e0,
               s0, halo0, o1, r1, sz, haloz, o0, r0,
               z0acc, d1acc, z1acc, gfacc,
               part, pair_in, rs_in, x_in, res,
               in_sem, out_sem, fwd_s, fwd_r, bwd_s, bwd_r, zs, zr, os_, or_,
               pair_s, pair_r, rs_s, rs_r, x_s, x_r, ag_s, ag_r, back_s, back_r):
        me = lax.axis_index("nodes")
        core = lax.rem(me, 2)
        x = lax.rem(me // 2, NX)
        plane = me // (2 * NX)

        def dev(i):
            return {"nodes": i}

        def plane_dev(i):
            return i * (2 * NX) + x * 2 + core

        def x_dev(i):
            return plane * (2 * NX) + i * 2 + core

        def near(o):
            return lax.rem(me + (o + n_dev), n_dev)

        mate = me + 1 - 2 * core

        loads = [pltpu.make_async_copy(a, b, in_sem.at[i]) for i, (a, b) in enumerate((
            (idx_hbm, idx), (h0_hbm, h0), (g_hbm, g), (w1_hbm, w1), (ahalo_hbm, ahalo), (aint_hbm, aint), (w0_hbm, w0)))]
        for cp in loads:
            cp.start()
        ld_idx, ld_h0, ld_g, ld_w1, ld_ahalo, ld_aint, ld_w0 = loads

        barrier = pltpu.get_barrier_semaphore()

        def sig(d):
            pl.semaphore_signal(barrier, inc=1, device_id=dev(d), device_id_type=pl.DeviceIdType.MESH)

        for o in OFFSETS:
            sig(near(o))
        sig(mate)

        def sig_x(p, c):
            sig(x_dev(lax.rem(x + p, NX)))
            return c

        def sig_p(p, c):
            sig(plane_dev(lax.rem(plane + p, PLANE)))
            return c

        lax.fori_loop(1, NX, sig_x, 0)
        lax.fori_loop(1, PLANE, sig_p, 0)

        def rcopy(src, dst, ss, rs, d):
            return pltpu.make_async_remote_copy(src_ref=src, dst_ref=dst, send_sem=ss, recv_sem=rs,
                                                device_id=dev(d), device_id_type=pl.DeviceIdType.MESH)

        def lanes(ref, k):
            return ref.at[:, pl.ds(k * slots, slots)]

        def link_copies(src, dst, ss, rs, sign):
            return [rcopy(lanes(src, k), lanes(dst, k), ss.at[k], rs.at[k], near(sign * OFFSETS[k])) for k in range(LINKS)]

        ld_idx.wait()
        rows = lax.broadcasted_iota(jnp.int32, (nodes, slots), 0)
        for k in range(LINKS):
            pt[:, k * slots:(k + 1) * slots] = jnp.where(rows == idx[k:k + 1, :], 1.0, 0.0).astype(BF16)
        ld_h0.wait()
        s0[...] = dot(h0[...], pt[...], 1, 0).astype(BF16)

        pl.semaphore_wait(barrier, LINKS + 1 + (NX - 1) + (PLANE - 1))
        fwd = link_copies(s0, halo0, fwd_s, fwd_r, 1)
        for cp in fwd:
            cp.start()

        ld_g.wait()
        ld_w1.wait()
        e1[...] = dot(w1[...], g[...], 0, 0).astype(BF16)
        ld_ahalo.wait()
        o1[...] = dot(e1[...], ahalo[...], 1, 0).astype(BF16)
        bwd = link_copies(o1, r1, bwd_s, bwd_r, -1)
        for cp in bwd:
            cp.start()

        ld_aint.wait()
        ld_w0.wait()
        z0acc[...] = dot(h0[...], aint[...], 1, 1)
        d1acc[...] = dot(e1[...], aint[...], 1, 0)

        for cp in fwd:
            cp.wait()
        z0[...] = (z0acc[...] + dot(halo0[...], ahalo[...], 1, 1)).astype(BF16)
        sz[...] = dot(z0[...], pt[...], 1, 0).astype(BF16)
        zcp = link_copies(sz, haloz, zs, zr, 1)
        for cp in zcp:
            cp.start()
        h1 = jnp.maximum(dot(w0[...], z0[...], 0, 0), 0.0).astype(BF16)
        ft[...] = h1
        z1acc[...] = dot(ft[...], aint[...], 1, 1)

        for cp in bwd:
            cp.wait()
        d1 = d1acc[...] + dot(r1[...], pt[...], 1, 1)
        ft[...] = jnp.where(ft[...] > 0, d1, 0.0).astype(BF16)

        part[...] = jnp.zeros_like(part)
        dw1 = dot(z0[...], ft[...], 1, 1)
        for s in range(n_slab):
            part[s // half_slabs, pl.ds((s % half_slabs) * slab1, feat), :] = dw1[:, s * 128:(s + 1) * 128]

        e0[...] = dot(w0[...], ft[...], 1, 0).astype(BF16)
        o0[...] = dot(e0[...], ahalo[...], 1, 0).astype(BF16)
        ocp = link_copies(o0, r0, os_, or_, -1)
        for cp in ocp:
            cp.start()

        for cp in zcp:
            cp.wait()
        h1h = jnp.maximum(dot(w0[...], haloz[...], 0, 0), 0.0).astype(BF16)
        z1 = (z1acc[...] + dot(h1h, ahalo[...], 1, 1)).astype(BF16)
        dw2 = dot(g[...], z1, 1, 1)
        for s in range(n_slab):
            part[s // half_slabs, pl.ds(off2 + (s % half_slabs) * slab2, cls), :] = dw2[:, s * 128:(s + 1) * 128]

        pair = rcopy(part.at[1 - core], pair_in, pair_s, pair_r, mate)
        pair.start()
        gfacc[...] = dot(e0[...], aint[...], 1, 0)
        pair.wait()
        part[core] = part[core] + pair_in[...]

        def rs_copy(p):
            i = lax.rem(plane + p, PLANE)
            return rcopy(part.at[core, pl.ds(pl.multiple_of(i * chunk, 8), chunk), :], rs_in.at[plane], rs_s.at[i], rs_r.at[plane], plane_dev(i))

        def rs_start(p, c):
            rs_copy(p).start()
            return c

        lax.fori_loop(1, PLANE, rs_start, 0)

        for cp in ocp:
            cp.wait()
        gfacc[...] = gfacc[...] + dot(r0[...], pt[...], 1, 1)
        gf_out = pltpu.make_async_copy(gfacc, gf_hbm, out_sem)
        gf_out.start()

        rs_in[plane] = part[core, pl.ds(pl.multiple_of(plane * chunk, 8), chunk), :]

        def rs_wait(p, c):
            i = lax.rem(plane + p, PLANE)
            cp = rcopy(part.at[core, pl.ds(pl.multiple_of(i * chunk, 8), chunk), :], rs_in.at[i], rs_s.at[i], rs_r.at[i], plane_dev(i))
            cp.wait()
            return c

        lax.fori_loop(1, PLANE, rs_wait, 0)
        total = rs_in[0]
        for i in range(1, PLANE):
            total = total + rs_in[i]
        x_in[x] = total

        def x_copy(i):
            return rcopy(x_in.at[x], x_in.at[x], x_s.at[i], x_r.at[x], x_dev(i))

        def x_start(p, c):
            x_copy(lax.rem(x + p, NX)).start()
            return c

        def x_wait(p, c):
            i = lax.rem(x + p, NX)
            rcopy(x_in.at[x], x_in.at[i], x_s.at[i], x_r.at[i], x_dev(i)).wait()
            return c

        lax.fori_loop(1, NX, x_start, 0)
        lax.fori_loop(1, NX, x_wait, 0)
        final = x_in[0]
        for i in range(1, NX):
            final = final + x_in[i]

        def own(i):
            return res.at[core, pl.ds(pl.multiple_of(i * chunk, 8), chunk), :]

        res[core, pl.ds(pl.multiple_of(plane * chunk, 8), chunk), :] = final

        def ag_start(p, c):
            i = lax.rem(plane + p, PLANE)
            rcopy(own(plane), own(plane), ag_s.at[i], ag_r.at[plane], plane_dev(i)).start()
            return c

        def ag_wait(p, c):
            i = lax.rem(plane + p, PLANE)
            rcopy(own(plane), own(i), ag_s.at[i], ag_r.at[i], plane_dev(i)).wait()
            return c

        lax.fori_loop(1, PLANE, ag_start, 0)
        lax.fori_loop(1, PLANE, ag_wait, 0)
        back = rcopy(res.at[core], res.at[core], back_s, back_r, mate)
        back.start()
        back_in = rcopy(res.at[core], res.at[1 - core], back_s, back_r, mate)
        back_in.wait()
        for s in range(n_slab):
            h, q = s // half_slabs, s % half_slabs
            dw1_out[:, s * 128:(s + 1) * 128] = res[h, pl.ds(q * slab1, feat), :]
            dw2_out[:, s * 128:(s + 1) * 128] = res[h, pl.ds(off2 + q * slab2, cls), :]
        gf_out.wait()

    V = pltpu.VMEM
    D = pltpu.SemaphoreType.DMA
    scratch = [
        V((feat, nodes), BF16), V((nodes, nodes), BF16), V((nodes, all_slots), BF16), V((LINKS, slots), jnp.int32),
        V((feat, hid), BF16), V((cls, hid), BF16), V((cls, nodes), BF16),
        V((nodes, all_slots), BF16), V((hid, nodes), BF16), V((feat, nodes), BF16), V((hid, nodes), BF16), V((feat, nodes), BF16),
        V((feat, all_slots), BF16), V((feat, all_slots), BF16), V((hid, all_slots), BF16), V((hid, all_slots), BF16),
        V((feat, all_slots), BF16), V((feat, all_slots), BF16), V((feat, all_slots), BF16), V((feat, all_slots), BF16),
        V((feat, nodes), F32), V((hid, nodes), F32), V((hid, nodes), F32), V((feat, nodes), F32),
        V((2, half, 128), F32), V((half, 128), F32), V((PLANE, chunk, 128), F32), V((NX, chunk, 128), F32), V((2, half, 128), F32),
        D((7,)), D, D((LINKS,)), D((LINKS,)), D((LINKS,)), D((LINKS,)), D((LINKS,)), D((LINKS,)), D((LINKS,)), D((LINKS,)),
        D, D, D((PLANE,)), D((PLANE,)), D((NX,)), D((NX,)), D((PLANE,)), D((PLANE,)), D, D,
    ]
    any_spec = pl.BlockSpec(memory_space=pl.ANY)
    vmem_spec = pl.BlockSpec(memory_space=pltpu.VMEM)
    return pl.pallas_call(
        kernel,
        out_shape=(jax.ShapeDtypeStruct((feat, hid), F32), jax.ShapeDtypeStruct((cls, hid), F32), jax.ShapeDtypeStruct((feat, nodes), F32)),
        in_specs=[any_spec] * 7,
        out_specs=(vmem_spec, vmem_spec, any_spec),
        scratch_shapes=scratch,
        compiler_params=pltpu.CompilerParams(collective_id=0, has_side_effects=True, vmem_limit_bytes=60 * 1024 * 1024),
        name="gcn_backward",
    )


def solution(mesh):
    axis_size = mesh.shape["nodes"]
    row_spec = P(("graph", "nodes"), None)
    replicated = P(None, None)
    part_spec = P("graph", None)

    def device_step(node_feats, a_int, a_halo, send_idx, w_first, w_second, grad_out):
        nodes, feat = node_feats.shape
        hid, cls = w_second.shape
        call = build(axis_size, nodes, feat, hid, cls, send_idx.shape[1])
        dw1, dw2, gf = call(node_feats.T, a_int, a_halo, send_idx, w_first, w_second.T, grad_out.T)
        return dw1, dw2.T, gf.T

    return jax.shard_map(device_step, mesh=mesh, in_specs=(row_spec, row_spec, row_spec, row_spec, replicated, replicated, row_spec), out_specs=(part_spec, part_spec, row_spec), check_vma=False)
```

```python
import jax
import jax.numpy as jnp
from jax import lax
from jax.experimental import pallas as pl
from jax.experimental.pallas import tpu as pltpu
from jax.sharding import PartitionSpec as P

F32 = jnp.float32
BF16 = jnp.bfloat16
NX, NY, NZ = 4, 4, 4
PLANE = NY * NZ
OFFSETS = (1, -1, 2, -2)
LINKS = 4


def dot(a, b, ca, cb):
    return lax.dot_general(a, b, (((ca,), (cb,)), ((), ())), preferred_element_type=F32)


def build(n_dev, nodes, feat, hid, cls, slots):
    all_slots = LINKS * slots
    slab1 = (feat + 7) // 8 * 8
    slab2 = (cls + 7) // 8 * 8
    n_slab = hid // 128
    half_slabs = n_slab // 2
    used = half_slabs * (slab1 + slab2)
    chunk = -(-used // (PLANE * 8)) * 8
    half = chunk * PLANE
    off2 = half_slabs * slab1

    def kernel(h0_hbm, aint_hbm, ahalo_hbm, idx_hbm, w0_hbm, w1_hbm, g_hbm,
               dw1_out, dw2_out, gf_out,
               h0, aint, ahalo, idx, w0, w1, g,
               pt, e1, z0, ft, e0,
               s0, halo0, o1, r1, sz, haloz, o0, r0,
               z0acc, d1acc, z1acc, gfacc,
               part, pair_in, rs_in, x_in, res,
               in_sem, fwd_s, fwd_r, bwd_s, bwd_r, zs, zr, os_, or_,
               pair_s, pair_r, rs_s, rs_r, x_s, x_r, ag_s, ag_r, back_s, back_r):
        me = lax.axis_index("nodes")
        core = lax.rem(me, 2)
        x = lax.rem(me // 2, NX)
        plane = me // (2 * NX)

        def dev(i):
            return {"nodes": i}

        def plane_dev(i):
            return i * (2 * NX) + x * 2 + core

        def x_dev(i):
            return plane * (2 * NX) + i * 2 + core

        def near(o):
            return lax.rem(me + (o + n_dev), n_dev)

        mate = me + 1 - 2 * core

        loads = [pltpu.make_async_copy(a, b, in_sem.at[i]) for i, (a, b) in enumerate((
            (idx_hbm, idx), (h0_hbm, h0), (g_hbm, g), (w1_hbm, w1), (ahalo_hbm, ahalo), (aint_hbm, aint), (w0_hbm, w0)))]
        for cp in loads:
            cp.start()
        ld_idx, ld_h0, ld_g, ld_w1, ld_ahalo, ld_aint, ld_w0 = loads

        barrier = pltpu.get_barrier_semaphore()

        def sig(d):
            pl.semaphore_signal(barrier, inc=1, device_id=dev(d), device_id_type=pl.DeviceIdType.MESH)

        for o in OFFSETS:
            sig(near(o))
        sig(mate)

        def sig_x(p, c):
            sig(x_dev(lax.rem(x + p, NX)))
            return c

        def sig_p(p, c):
            sig(plane_dev(lax.rem(plane + p, PLANE)))
            return c

        lax.fori_loop(1, NX, sig_x, 0)
        lax.fori_loop(1, PLANE, sig_p, 0)

        def rcopy(src, dst, ss, rs, d):
            return pltpu.make_async_remote_copy(src_ref=src, dst_ref=dst, send_sem=ss, recv_sem=rs,
                                                device_id=dev(d), device_id_type=pl.DeviceIdType.MESH)

        def lanes(ref, k):
            return ref.at[:, pl.ds(k * slots, slots)]

        def link_copies(src, dst, ss, rs, sign):
            return [rcopy(lanes(src, k), lanes(dst, k), ss.at[k], rs.at[k], near(sign * OFFSETS[k])) for k in range(LINKS)]

        ld_idx.wait()
        rows = lax.broadcasted_iota(jnp.int32, (nodes, slots), 0)
        for k in range(LINKS):
            pt[:, k * slots:(k + 1) * slots] = jnp.where(rows == idx[k:k + 1, :], 1.0, 0.0).astype(BF16)
        ld_h0.wait()
        s0[...] = dot(h0[...], pt[...], 1, 0).astype(BF16)

        pl.semaphore_wait(barrier, LINKS + 1 + (NX - 1) + (PLANE - 1))
        fwd = link_copies(s0, halo0, fwd_s, fwd_r, 1)
        for cp in fwd:
            cp.start()

        ld_g.wait()
        ld_w1.wait()
        e1[...] = dot(w1[...], g[...], 0, 0).astype(BF16)
        ld_ahalo.wait()
        o1[...] = dot(e1[...], ahalo[...], 1, 0).astype(BF16)
        bwd = link_copies(o1, r1, bwd_s, bwd_r, -1)
        for cp in bwd:
            cp.start()

        ld_aint.wait()
        ld_w0.wait()
        z0acc[...] = dot(h0[...], aint[...], 1, 1)
        d1acc[...] = dot(e1[...], aint[...], 1, 0)

        for cp in fwd:
            cp.wait()
        z0[...] = (z0acc[...] + dot(halo0[...], ahalo[...], 1, 1)).astype(BF16)
        sz[...] = dot(z0[...], pt[...], 1, 0).astype(BF16)
        zcp = link_copies(sz, haloz, zs, zr, 1)
        for cp in zcp:
            cp.start()
        h1 = jnp.maximum(dot(w0[...], z0[...], 0, 0), 0.0).astype(BF16)
        ft[...] = h1
        z1acc[...] = dot(ft[...], aint[...], 1, 1)

        for cp in bwd:
            cp.wait()
        d1 = d1acc[...] + dot(r1[...], pt[...], 1, 1)
        ft[...] = jnp.where(ft[...] > 0, d1, 0.0).astype(BF16)

        part[...] = jnp.zeros_like(part)
        dw1 = dot(z0[...], ft[...], 1, 1)
        for s in range(n_slab):
            part[s // half_slabs, pl.ds((s % half_slabs) * slab1, feat), :] = dw1[:, s * 128:(s + 1) * 128]

        e0[...] = dot(w0[...], ft[...], 1, 0).astype(BF16)
        o0[...] = dot(e0[...], ahalo[...], 1, 0).astype(BF16)
        ocp = link_copies(o0, r0, os_, or_, -1)
        for cp in ocp:
            cp.start()

        for cp in zcp:
            cp.wait()
        h1h = jnp.maximum(dot(w0[...], haloz[...], 0, 0), 0.0).astype(BF16)
        z1 = (z1acc[...] + dot(h1h, ahalo[...], 1, 1)).astype(BF16)
        dw2 = dot(g[...], z1, 1, 1)
        for s in range(n_slab):
            part[s // half_slabs, pl.ds(off2 + (s % half_slabs) * slab2, cls), :] = dw2[:, s * 128:(s + 1) * 128]

        pair = rcopy(part.at[1 - core], pair_in, pair_s, pair_r, mate)
        pair.start()
        gfacc[...] = dot(e0[...], aint[...], 1, 0)
        pair.wait()
        part[core] = part[core] + pair_in[...]

        def rs_copy(p):
            i = lax.rem(plane + p, PLANE)
            return rcopy(part.at[core, pl.ds(pl.multiple_of(i * chunk, 8), chunk), :], rs_in.at[plane], rs_s.at[i], rs_r.at[plane], plane_dev(i))

        def rs_start(p, c):
            rs_copy(p).start()
            return c

        lax.fori_loop(1, PLANE, rs_start, 0)

        for cp in ocp:
            cp.wait()
        gf_out[...] = gfacc[...] + dot(r0[...], pt[...], 1, 1)

        rs_in[plane] = part[core, pl.ds(pl.multiple_of(plane * chunk, 8), chunk), :]

        def rs_wait(p, c):
            i = lax.rem(plane + p, PLANE)
            cp = rcopy(part.at[core, pl.ds(pl.multiple_of(i * chunk, 8), chunk), :], rs_in.at[i], rs_s.at[i], rs_r.at[i], plane_dev(i))
            cp.wait()
            return c

        lax.fori_loop(1, PLANE, rs_wait, 0)
        total = rs_in[0]
        for i in range(1, PLANE):
            total = total + rs_in[i]
        x_in[x] = total

        def x_copy(i):
            return rcopy(x_in.at[x], x_in.at[x], x_s.at[i], x_r.at[x], x_dev(i))

        def x_start(p, c):
            x_copy(lax.rem(x + p, NX)).start()
            return c

        def x_wait(p, c):
            i = lax.rem(x + p, NX)
            rcopy(x_in.at[x], x_in.at[i], x_s.at[i], x_r.at[i], x_dev(i)).wait()
            return c

        lax.fori_loop(1, NX, x_start, 0)
        lax.fori_loop(1, NX, x_wait, 0)
        final = x_in[0]
        for i in range(1, NX):
            final = final + x_in[i]

        def own(i):
            return res.at[core, pl.ds(pl.multiple_of(i * chunk, 8), chunk), :]

        res[core, pl.ds(pl.multiple_of(plane * chunk, 8), chunk), :] = final

        def ag_start(p, c):
            i = lax.rem(plane + p, PLANE)
            rcopy(own(plane), own(plane), ag_s.at[i], ag_r.at[plane], plane_dev(i)).start()
            return c

        def ag_wait(p, c):
            i = lax.rem(plane + p, PLANE)
            rcopy(own(plane), own(i), ag_s.at[i], ag_r.at[i], plane_dev(i)).wait()
            return c

        lax.fori_loop(1, PLANE, ag_start, 0)
        lax.fori_loop(1, PLANE, ag_wait, 0)
        back = rcopy(res.at[core], res.at[core], back_s, back_r, mate)
        back.start()
        back_in = rcopy(res.at[core], res.at[1 - core], back_s, back_r, mate)
        back_in.wait()
        for s in range(n_slab):
            h, q = s // half_slabs, s % half_slabs
            dw1_out[:, s * 128:(s + 1) * 128] = res[h, pl.ds(q * slab1, feat), :]
            dw2_out[:, s * 128:(s + 1) * 128] = res[h, pl.ds(off2 + q * slab2, cls), :]

    V = pltpu.VMEM
    D = pltpu.SemaphoreType.DMA
    scratch = [
        V((feat, nodes), BF16), V((nodes, nodes), BF16), V((nodes, all_slots), BF16), V((LINKS, slots), jnp.int32),
        V((feat, hid), BF16), V((cls, hid), BF16), V((cls, nodes), BF16),
        V((nodes, all_slots), BF16), V((hid, nodes), BF16), V((feat, nodes), BF16), V((hid, nodes), BF16), V((feat, nodes), BF16),
        V((feat, all_slots), BF16), V((feat, all_slots), BF16), V((hid, all_slots), BF16), V((hid, all_slots), BF16),
        V((feat, all_slots), BF16), V((feat, all_slots), BF16), V((feat, all_slots), BF16), V((feat, all_slots), BF16),
        V((feat, nodes), F32), V((hid, nodes), F32), V((hid, nodes), F32), V((feat, nodes), F32),
        V((2, half, 128), F32), V((half, 128), F32), V((PLANE, chunk, 128), F32), V((NX, chunk, 128), F32), V((2, half, 128), F32),
        D((7,)), D((LINKS,)), D((LINKS,)), D((LINKS,)), D((LINKS,)), D((LINKS,)), D((LINKS,)), D((LINKS,)), D((LINKS,)),
        D, D, D((PLANE,)), D((PLANE,)), D((NX,)), D((NX,)), D((PLANE,)), D((PLANE,)), D, D,
    ]
    any_spec = pl.BlockSpec(memory_space=pl.ANY)
    vmem_spec = pl.BlockSpec(memory_space=pltpu.VMEM)
    return pl.pallas_call(
        kernel,
        out_shape=(pltpu.VMEM((feat, hid), F32), pltpu.VMEM((cls, hid), F32), pltpu.VMEM((feat, nodes), F32)),
        in_specs=[any_spec] * 7,
        out_specs=(vmem_spec, vmem_spec, vmem_spec),
        scratch_shapes=scratch,
        compiler_params=pltpu.CompilerParams(collective_id=0, has_side_effects=True, vmem_limit_bytes=64897024),
        name="gcn_backward",
    )


def write_out(feat, hid, cls, nodes):
    def kernel(dw1, dw2, gf, dw1_out, dw2_out, gf_out, sems):
        copies = [pltpu.make_async_copy(a, b, sems.at[i]) for i, (a, b) in enumerate(((gf, gf_out), (dw1, dw1_out), (dw2, dw2_out)))]
        for cp in copies:
            cp.start()
        for cp in copies:
            cp.wait()

    return pl.pallas_call(
        kernel,
        out_shape=(jax.ShapeDtypeStruct((feat, hid), F32), jax.ShapeDtypeStruct((cls, hid), F32), jax.ShapeDtypeStruct((feat, nodes), F32)),
        in_specs=[pl.BlockSpec(memory_space=pltpu.VMEM)] * 3,
        out_specs=(pl.BlockSpec(memory_space=pl.ANY),) * 3,
        scratch_shapes=[pltpu.SemaphoreType.DMA((3,))],
        compiler_params=pltpu.CompilerParams(vmem_limit_bytes=4 * 1024 * 1024),
        name="write_out",
    )


def solution(mesh):
    axis_size = mesh.shape["nodes"]
    row_spec = P(("graph", "nodes"), None)
    replicated = P(None, None)
    part_spec = P("graph", None)

    def device_step(node_feats, a_int, a_halo, send_idx, w_first, w_second, grad_out):
        nodes, feat = node_feats.shape
        hid, cls = w_second.shape
        call = build(axis_size, nodes, feat, hid, cls, send_idx.shape[1])
        dw1, dw2, gf = call(node_feats.T, a_int, a_halo, send_idx, w_first, w_second.T, grad_out.T)
        dw1, dw2, gf = write_out(feat, hid, cls, nodes)(dw1, dw2, gf)
        return dw1, dw2.T, gf.T

    return jax.shard_map(device_step, mesh=mesh, in_specs=(row_spec, row_spec, row_spec, row_spec, replicated, replicated, row_spec), out_specs=(part_spec, part_spec, row_spec), check_vma=False)
```

```python
import jax
import jax.numpy as jnp
from jax import lax
from jax.experimental import pallas as pl
from jax.experimental.pallas import tpu as pltpu
from jax.sharding import PartitionSpec as P

F32 = jnp.float32
BF16 = jnp.bfloat16
SIDE = 4
PLANE = SIDE * SIDE
CUBE = PLANE * SIDE
OFFSETS = (1, -1, 2, -2)
LINKS = 4
VMEM_BYTES = 67043328


def dot(a, b, ca, cb):
    return lax.dot_general(a, b, (((ca,), (cb,)), ((), ())), preferred_element_type=F32)


def hops(step):
    return sum(min(d, SIDE - d) for d in step)


PLANE_PEERS = sorted(((a, b) for a in range(SIDE) for b in range(SIDE) if a or b), key=hops, reverse=True)
CUBE_PEERS = sorted(((a, b, c) for a in range(SIDE) for b in range(SIDE) for c in range(SIDE) if a or b or c), key=hops, reverse=True)


class Piece:
    def __init__(self, num, plane, cross, rows, base):
        self.num, self.plane, self.cross, self.rows, self.base = num, plane, cross, rows, base

    def steps(self, ab):
        st = [0, 0, 0]
        st[self.plane[0]], st[self.plane[1]] = ab
        return tuple(st)

    def across(self, step):
        st = [0, 0, 0]
        st[self.cross] = step
        return tuple(st)


def build(n_dev, nodes, feat, hid, cls, slots):
    all_slots = LINKS * slots
    half_hid = hid // 2
    n_slab = hid // 128
    slab1 = (feat + 7) // 8 * 8
    slab2 = (cls + 7) // 8 * 8
    half_rows = n_slab // 2 * slab1
    units = -(-half_rows // (PLANE * 8))
    share = [8 * ((units + 2 - p) // 3) for p in range(3)]
    pieces, end1 = [], 0
    for num, (dims, rows) in enumerate(zip((((1, 2), 0), ((0, 1), 2), ((0, 2), 1)), share)):
        pieces.append(Piece(num, dims[0], dims[1], rows, end1))
        end1 += rows * PLANE
    rows1 = sum(share)
    rows2 = -(-n_slab * slab2 // (CUBE * 8)) * 8
    end2 = rows2 * CUBE

    def kernel(h0_hbm, aint_hbm, ahalo_hbm, idx_hbm, w0_hbm, w1_hbm, g_hbm,
               dw1_out, dw2_out, gf_out,
               h0, aint, ahalo, idx, w0, w1, g,
               pt, e1, z0, ft, e0,
               s0, halo0, o1, r1, sz, haloz, o0, r0,
               z0acc, d1acc, z1acc, gfacc,
               part1, part2, pair1_in, pair2_in, rs1_in, rs2_in, x_in, res1, res2,
               in_sem, fwd_sem, bwd_sem, zcp_sem, ocp_sem,
               pair1_sem, pair2_sem, rs1_sem, rs2_sem, x_sem, ag1_s, ag1_r, ag2_s, ag2_r, back1_sem, back2_sem, gossip):
        me = lax.axis_index("nodes")
        core = lax.rem(me, 2)
        coord = (lax.rem(me // 2, SIDE), lax.rem(me // (2 * SIDE), SIDE), me // (2 * SIDE * SIDE))
        stride = (2, 2 * SIDE, 2 * SIDE * SIDE)
        mate = me + 1 - 2 * core

        def moved(dim, step):
            return lax.rem(coord[dim] + step, SIDE)

        def peer(steps):
            d = core
            for dim in range(3):
                d = d + moved(dim, steps[dim]) * stride[dim]
            return d

        def near(o):
            return lax.rem(me + (o + n_dev), n_dev)

        def signal(sem, d):
            pl.semaphore_signal(sem, inc=1, device_id={"nodes": d}, device_id_type=pl.DeviceIdType.MESH)

        def rcopy(src, dst, ss, rs, d):
            return pltpu.make_async_remote_copy(src_ref=src, dst_ref=dst, send_sem=ss, recv_sem=rs,
                                                device_id={"nodes": d}, device_id_type=pl.DeviceIdType.MESH)

        def lanes(ref, k):
            return ref.at[:, pl.ds(k * slots, slots)]

        def link_copies(src, dst, sems, sign):
            return [rcopy(lanes(src, k), lanes(dst, k), sems.at[0, k // 2], sems.at[1, k // 2], near(sign * OFFSETS[k])) for k in range(LINKS)]

        def link_wait(src, dst, sems, i):
            both = pl.ds(2 * i * slots, 2 * slots)
            rcopy(src.at[:, both], dst.at[:, both], sems.at[0, i], sems.at[1, i], mate).wait()

        def start(copies):
            for cp in copies:
                cp.start()

        def wait(copies):
            for cp in copies:
                cp.wait()

        loads = [pltpu.make_async_copy(a, b, in_sem.at[i]) for i, (a, b) in enumerate((
            (idx_hbm, idx), (h0_hbm, h0), (g_hbm, g), (w1_hbm, w1), (ahalo_hbm, ahalo), (aint_hbm, aint), (w0_hbm, w0)))]
        start(loads)
        ld_idx, ld_h0, ld_g, ld_w1, ld_ahalo, ld_aint, ld_w0 = loads
        barrier = pltpu.get_barrier_semaphore()
        ring = [peer(tuple(step if d == dim else 0 for d in range(3))) for dim in range(3) for step in (1, SIDE - 1)]
        greeted = [near(o) for o in OFFSETS] + [mate] + ring
        for d in greeted:
            signal(barrier, d)

        def gossip_send(i):
            for d in ring:
                signal(gossip.at[i], d)

        def gossip_wait(i):
            pl.semaphore_wait(gossip.at[i], len(ring))

        part1[...] = jnp.zeros_like(part1)
        part2[...] = jnp.zeros_like(part2)
        node_id = lax.broadcasted_iota(jnp.int32, (nodes, slots), 0)
        fwd = link_copies(s0, halo0, fwd_sem, 1)
        bwd = link_copies(o1, r1, bwd_sem, -1)
        zcp = link_copies(sz, haloz, zcp_sem, 1)
        ocp = link_copies(o0, r0, ocp_sem, -1)
        upper = pl.ds(2 * slots, 2 * slots)
        lower = pl.ds(0, 2 * slots)

        def select_rows(ks):
            for k in ks:
                pt[:, k * slots:(k + 1) * slots] = jnp.where(node_id == idx[k:k + 1, :], 1.0, 0.0).astype(BF16)

        with jax.named_scope("ld_idx"):
            ld_idx.wait()
        with jax.named_scope("pt"):
            select_rows((2, 3))
        with jax.named_scope("ld_h0"):
            ld_h0.wait()
        with jax.named_scope("s0"):
            s0[:, upper] = dot(h0[...], pt[:, upper], 1, 0).astype(BF16)
        with jax.named_scope("barrier"):
            pl.semaphore_wait(barrier, len(greeted))
        with jax.named_scope("fwd_start"):
            start(fwd[2:])
        with jax.named_scope("s0_low"):
            select_rows((0, 1))
            s0[:, lower] = dot(h0[...], pt[:, lower], 1, 0).astype(BF16)
        with jax.named_scope("fwd_start_low"):
            start(fwd[:2])
            gossip_send(0)
        with jax.named_scope("e1"):
            ld_g.wait()
            ld_w1.wait()
            e1[...] = dot(w1[...], g[...], 0, 0).astype(BF16)
        with jax.named_scope("o1"):
            ld_ahalo.wait()
            o1[...] = dot(e1[...], ahalo[...], 1, 0).astype(BF16)
        with jax.named_scope("bwd_start"):
            start(bwd[2:] + bwd[:2])
        with jax.named_scope("z0acc"):
            ld_aint.wait()
            z0acc[...] = dot(h0[...], aint[...], 1, 1)
        with jax.named_scope("gossip0"):
            gossip_wait(0)
            gossip_send(1)
        with jax.named_scope("d1acc"):
            d1acc[...] = dot(e1[...], aint[...], 1, 0)

        with jax.named_scope("fwd_wait"):
            link_wait(s0, halo0, fwd_sem, 0)
            link_wait(s0, halo0, fwd_sem, 1)
        with jax.named_scope("z0"):
            z0[...] = (z0acc[...] + dot(halo0[...], ahalo[...], 1, 1)).astype(BF16)
        with jax.named_scope("sz"):
            sz[...] = dot(z0[...], pt[...], 1, 0).astype(BF16)
        with jax.named_scope("z_start"):
            start(zcp[2:] + zcp[:2])
        with jax.named_scope("gossip1"):
            gossip_wait(1)
            gossip_send(2)
        with jax.named_scope("h1"):
            ld_w0.wait()
            ft[...] = jnp.maximum(dot(w0[...], z0[...], 0, 0), 0.0).astype(BF16)
        with jax.named_scope("z1acc"):
            z1acc[...] = dot(ft[...], aint[...], 1, 1)
        with jax.named_scope("gossip2"):
            gossip_wait(2)
            gossip_send(3)

        with jax.named_scope("bwd_wait_up"):
            link_wait(o1, r1, bwd_sem, 1)
        with jax.named_scope("d1_up"):
            d1acc[...] = d1acc[...] + dot(r1[:, upper], pt[:, upper], 1, 1)
        with jax.named_scope("bwd_wait_low"):
            link_wait(o1, r1, bwd_sem, 0)

        def first_half(h):
            rows = pl.ds(pl.multiple_of(h * half_hid, half_hid), half_hid)
            d1 = d1acc[rows, :] + dot(r1[rows, lower], pt[:, lower], 1, 1)
            ft[rows, :] = jnp.where(ft[rows, :] > 0, d1, 0.0).astype(BF16)
            dw1 = dot(z0[...], ft[rows, :], 1, 1)
            for s in range(half_hid // 128):
                part1[h, pl.ds(s * slab1, feat), :] = dw1[:, s * 128:(s + 1) * 128]

        def rows_of(ref, n, i):
            return ref.at[pl.ds(pl.multiple_of(i * n, 8), n), :]

        def rows_wait(ref, rows, ss, rs):
            some = ref.at[pl.ds(0, rows), :]
            if ss is not None:
                rcopy(some, some, ss, ss, mate).wait_send()
            if rs is not None:
                rcopy(some, some, rs, rs, mate).wait_recv()

        pair1 = rcopy(part1.at[1 - core, pl.ds(0, half_rows), :], pair1_in, pair1_sem.at[0], pair1_sem.at[1], mate)

        def plane_id(p, ab=(0, 0)):
            return moved(p.plane[0], ab[0]) * SIDE + moved(p.plane[1], ab[1])

        def chunk1(ref, p, i):
            return ref.at[core, pl.ds(pl.multiple_of(p.base + i * p.rows, 8), p.rows), :]

        def stage(ref, p, i):
            return ref.at[p.num, i, pl.ds(0, p.rows), :]

        def rs1_send(group):
            start([rcopy(chunk1(part1, p, plane_id(p, ab)), stage(rs1_in, p, plane_id(p)), rs1_sem.at[0], rs1_sem.at[1], peer(p.steps(ab)))
                   for ab in PLANE_PEERS for p in group])
            for p in group:
                rs1_in[p.num, plane_id(p), pl.ds(0, p.rows), :] = part1[core, pl.ds(pl.multiple_of(p.base + plane_id(p) * p.rows, 8), p.rows), :]

        def rs1_start():
            used = pl.ds(0, half_rows)
            part1[core, used, :] = part1[core, used, :] + pair1_in[...]
            rs1_send(pieces[:1])

        def rs1_finish():
            rows_wait(part1.at[0], (PLANE - 1) * rows1, rs1_sem.at[0], rs1_sem.at[1])
            for p in pieces:
                total = rs1_in[p.num, 0, 0:p.rows, :]
                for i in range(1, PLANE):
                    total = total + rs1_in[p.num, i, 0:p.rows, :]
                x_in[p.num, coord[p.cross], pl.ds(0, p.rows), :] = total
            start([rcopy(stage(x_in, p, coord[p.cross]), stage(x_in, p, coord[p.cross]), x_sem.at[0], x_sem.at[1], peer(p.across(step)))
                   for step in (2, 1, 3) for p in pieces])

        def x1_finish():
            rows_wait(part1.at[0], (SIDE - 1) * rows1, x_sem.at[0], x_sem.at[1])
            for p in pieces:
                total = x_in[p.num, 0, 0:p.rows, :]
                for i in range(1, SIDE):
                    total = total + x_in[p.num, i, 0:p.rows, :]
                res1[core, pl.ds(pl.multiple_of(p.base + plane_id(p) * p.rows, 8), p.rows), :] = total
            start([rcopy(chunk1(res1, p, plane_id(p)), chunk1(res1, p, plane_id(p)), ag1_s, ag1_r.at[hops(ab) - 1], peer(p.steps(ab)))
                   for ab in PLANE_PEERS for p in pieces])
            start([back1(p, plane_id(p)) for p in pieces])

        def back1(p, i):
            return rcopy(chunk1(res1, p, i), chunk1(res1, p, i), back1_sem.at[0], back1_sem.at[1], mate)

        def ag1_finish():
            for n in range(1, 5):
                near_n = [ab for ab in PLANE_PEERS if hops(ab) == n]
                rows_wait(part1.at[0], len(near_n) * rows1, None, ag1_r.at[n - 1])
                start([back1(p, plane_id(p, ab)) for ab in near_n for p in pieces])
            rows_wait(part1.at[0], (PLANE - 1) * rows1, ag1_s, None)

        def back1_finish():
            rows_wait(part1.at[0], PLANE * rows1, back1_sem.at[0], back1_sem.at[1])

        my_cube = coord[0] + SIDE * (coord[1] + SIDE * coord[2])
        pair2 = rcopy(part2.at[pl.ds(0, n_slab * slab2), :], pair2_in, pair2_sem.at[0], pair2_sem.at[1], mate)

        def cube_id(steps):
            return moved(0, steps[0]) + SIDE * (moved(1, steps[1]) + SIDE * moved(2, steps[2]))

        def rs2_start():
            pair2.wait_recv()
            used = pl.ds(0, n_slab * slab2)
            part2[used, :] = part2[used, :] + pair2_in[...]
            start([rcopy(rows_of(part2, rows2, cube_id(st)), rs2_in.at[my_cube], rs2_sem.at[0], rs2_sem.at[1], peer(st)) for st in CUBE_PEERS])
            rs2_in[my_cube] = part2[pl.ds(pl.multiple_of(my_cube * rows2, 8), rows2), :]

        def rs2_finish():
            rows_wait(part2, (CUBE - 1) * rows2, rs2_sem.at[0], rs2_sem.at[1])
            sums = [rs2_in[i] for i in range(CUBE)]
            while len(sums) > 1:
                sums = [a + b for a, b in zip(sums[::2], sums[1::2])]
            res2[pl.ds(pl.multiple_of(my_cube * rows2, 8), rows2), :] = sums[0]
            mine = rows_of(res2, rows2, my_cube)
            start([rcopy(mine, mine, ag2_s, ag2_r.at[hops(st) - 1], peer(st)) for st in CUBE_PEERS])
            back2(my_cube).start()

        def back2(i):
            return rcopy(rows_of(res2, rows2, i), rows_of(res2, rows2, i), back2_sem.at[0], back2_sem.at[1], mate)

        def ag2_finish():
            for n in range(1, 7):
                near_n = [st for st in CUBE_PEERS if hops(st) == n]
                rows_wait(part2, len(near_n) * rows2, None, ag2_r.at[n - 1])
                start([back2(cube_id(st)) for st in near_n])
            rows_wait(part2, (CUBE - 1) * rows2, ag2_s, None)
            rows_wait(part2, CUBE * rows2, back2_sem.at[0], None)

        def on(which, name, *steps):
            @pl.when(core == which)
            def _():
                with jax.named_scope(name):
                    for step in steps:
                        step()

        def run(name, *steps):
            with jax.named_scope(name):
                for step in steps:
                    step()

        run("half_mate", lambda: first_half(1 - core))
        run("pair1_start", pair1.start)
        run("half_own", lambda: first_half(core))
        with jax.named_scope("e0"):
            e0[...] = dot(w0[...], ft[...], 1, 0).astype(BF16)
        with jax.named_scope("gossip3"):
            gossip_wait(3)
            gossip_send(4)
        run("pair1_wait", pair1.wait)
        run("rs1_start", rs1_start)
        with jax.named_scope("o0"):
            o0[...] = dot(e0[...], ahalo[...], 1, 0).astype(BF16)

        with jax.named_scope("z_wait"):
            link_wait(sz, haloz, zcp_sem, 0)
            link_wait(sz, haloz, zcp_sem, 1)
        run("rs1_start_x", lambda: rs1_send(pieces[1:]))
        with jax.named_scope("h1h"):
            h1h = jnp.maximum(dot(w0[...], haloz[...], 0, 0), 0.0).astype(BF16)
        with jax.named_scope("z1"):
            z1 = (z1acc[...] + dot(h1h, ahalo[...], 1, 1)).astype(BF16)
        with jax.named_scope("dw2"):
            dw2 = dot(g[...], z1, 1, 1)
            for s in range(n_slab):
                part2[pl.ds(s * slab2, cls), :] = dw2[:, s * 128:(s + 1) * 128]
        on(0, "pair2_start", pair2.start)
        with jax.named_scope("o_start"):
            start(ocp)
            gossip_wait(4)
        with jax.named_scope("gfacc"):
            gfacc[...] = dot(e0[...], aint[...], 1, 0)
        on(1, "rs2_start", rs2_start)
        run("rs1_finish", rs1_finish)
        with jax.named_scope("o_wait"):
            link_wait(o0, r0, ocp_sem, 0)
            link_wait(o0, r0, ocp_sem, 1)
        with jax.named_scope("gf"):
            gf_out[...] = gfacc[...] + dot(r0[...], pt[...], 1, 1)
        run("x1_finish", x1_finish)
        on(1, "rs2_finish", rs2_finish)
        run("ag1_finish", ag1_finish)
        on(1, "ag2_finish", ag2_finish)
        run("back1_finish", back1_finish)
        on(0, "back2_wait", lambda: rows_wait(part2, CUBE * rows2, None, back2_sem.at[1]), pair2.wait_send)
        with jax.named_scope("outs"):
            for s in range(n_slab):
                h, q = s // (n_slab // 2), s % (n_slab // 2)
                dw1_out[:, s * 128:(s + 1) * 128] = res1[h, pl.ds(q * slab1, feat), :]
                dw2_out[:, s * 128:(s + 1) * 128] = res2[pl.ds(s * slab2, cls), :]

    V = pltpu.VMEM
    D = pltpu.SemaphoreType.DMA
    link_sems = [D((2, 2))] * 4
    scratch = [
        V((feat, nodes), BF16), V((nodes, nodes), BF16), V((nodes, all_slots), BF16), V((LINKS, slots), jnp.int32),
        V((feat, hid), BF16), V((cls, hid), BF16), V((cls, nodes), BF16),
        V((nodes, all_slots), BF16), V((hid, nodes), BF16), V((feat, nodes), BF16), V((hid, nodes), BF16), V((feat, nodes), BF16),
        V((feat, all_slots), BF16), V((feat, all_slots), BF16), V((hid, all_slots), BF16), V((hid, all_slots), BF16),
        V((feat, all_slots), BF16), V((feat, all_slots), BF16), V((feat, all_slots), BF16), V((feat, all_slots), BF16),
        V((feat, nodes), F32), V((hid, nodes), F32), V((hid, nodes), F32), V((feat, nodes), F32),
        V((2, end1, 128), F32), V((end2, 128), F32), V((half_rows, 128), F32), V((n_slab * slab2, 128), F32),
        V((3, PLANE, max(share), 128), F32), V((CUBE, rows2, 128), F32), V((3, SIDE, max(share), 128), F32), V((2, end1, 128), F32), V((end2, 128), F32),
        D((7,)), *link_sems, D((2,)), D((2,)), D((2,)), D((2,)), D((2,)), D, D((4,)), D, D((6,)), D((2,)), D((2,)), pltpu.SemaphoreType.REGULAR((5,)),
    ]
    out_bytes = 4 * (slab1 * hid + slab2 * hid + slab1 * nodes)
    any_spec = pl.BlockSpec(memory_space=pl.ANY)
    vmem_spec = pl.BlockSpec(memory_space=pltpu.VMEM)
    return pl.pallas_call(
        kernel,
        out_shape=(pltpu.VMEM((feat, hid), F32), pltpu.VMEM((cls, hid), F32), pltpu.VMEM((feat, nodes), F32)),
        in_specs=[any_spec] * 7,
        out_specs=(vmem_spec, vmem_spec, vmem_spec),
        scratch_shapes=scratch,
        compiler_params=pltpu.CompilerParams(collective_id=0, has_side_effects=True, vmem_limit_bytes=VMEM_BYTES - out_bytes - 65536),
        name="gcn_backward",
    )


def write_out(feat, hid, cls, nodes):
    def kernel(dw1, dw2, gf, dw1_out, dw2_out, gf_out, sems):
        copies = [pltpu.make_async_copy(a, b, sems.at[i]) for i, (a, b) in enumerate(((gf, gf_out), (dw1, dw1_out), (dw2, dw2_out)))]
        for cp in copies:
            cp.start()
        for cp in copies:
            cp.wait()

    return pl.pallas_call(
        kernel,
        out_shape=(jax.ShapeDtypeStruct((feat, hid), F32), jax.ShapeDtypeStruct((cls, hid), F32), jax.ShapeDtypeStruct((feat, nodes), F32)),
        in_specs=[pl.BlockSpec(memory_space=pltpu.VMEM)] * 3,
        out_specs=(pl.BlockSpec(memory_space=pl.ANY),) * 3,
        scratch_shapes=[pltpu.SemaphoreType.DMA((3,))],
        compiler_params=pltpu.CompilerParams(vmem_limit_bytes=4 * 1024 * 1024),
        name="write_out",
    )


def solution(mesh):
    axis_size = mesh.shape["nodes"]
    row_spec = P(("graph", "nodes"), None)
    replicated = P(None, None)
    part_spec = P("graph", None)

    def device_step(node_feats, a_int, a_halo, send_idx, w_first, w_second, grad_out):
        nodes, feat = node_feats.shape
        hid, cls = w_second.shape
        call = build(axis_size, nodes, feat, hid, cls, send_idx.shape[1])
        dw1, dw2, gf = call(node_feats.T, a_int, a_halo, send_idx, w_first, w_second.T, grad_out.T)
        dw1, dw2, gf = write_out(feat, hid, cls, nodes)(dw1, dw2, gf)
        return dw1, dw2.T, gf.T

    return jax.shard_map(device_step, mesh=mesh, in_specs=(row_spec, row_spec, row_spec, row_spec, replicated, replicated, row_spec), out_specs=(part_spec, part_spec, row_spec), check_vma=False)
```

```python
import jax
import jax.numpy as jnp
from jax import lax
from jax.experimental import pallas as pl
from jax.experimental.pallas import tpu as pltpu
from jax.sharding import PartitionSpec as P

F32 = jnp.float32
BF16 = jnp.bfloat16
SIDE = 4
PLANE = SIDE * SIDE
CUBE = PLANE * SIDE
OFFSETS = (1, -1, 2, -2)
LINKS = 4
VMEM_BYTES = 67043328
WRITES = 4


def dot(a, b, ca, cb):
    return lax.dot_general(a, b, (((ca,), (cb,)), ((), ())), preferred_element_type=F32)


def hops(step):
    return sum(min(d, SIDE - d) for d in step)


PLANE_PEERS = sorted(((a, b) for a in range(SIDE) for b in range(SIDE) if a or b), key=hops, reverse=True)
CUBE_PEERS = sorted(((a, b, c) for a in range(SIDE) for b in range(SIDE) for c in range(SIDE) if a or b or c), key=hops, reverse=True)


RELEASE = ((0.0, 0.5, 0.9, 1.1), (0.0, 0.6, 1.2, 1.4), (0.0, 0.9, 1.8, 2.4))


def release_order(dims):
    spots = [()]
    for _ in dims:
        spots = [s + (c,) for s in spots for c in range(SIDE)]
    return sorted(spots, key=lambda s: sum(RELEASE[d][c] for d, c in zip(dims, s)))


class Piece:
    def __init__(self, num, plane, cross, rows, base):
        self.num, self.plane, self.cross, self.rows, self.base = num, plane, cross, rows, base

    def steps(self, ab):
        st = [0, 0, 0]
        st[self.plane[0]], st[self.plane[1]] = ab
        return tuple(st)

    def across(self, step):
        st = [0, 0, 0]
        st[self.cross] = step
        return tuple(st)


def build(n_dev, nodes, feat, hid, cls, slots):
    all_slots = LINKS * slots
    half_hid = hid // 2
    n_slab = hid // 128
    slab1 = (feat + 7) // 8 * 8
    slab2 = (cls + 7) // 8 * 8
    half_rows = n_slab // 2 * slab1
    units = -(-half_rows // (PLANE * 8))
    share = [8 * ((units + 2 - p) // 3) for p in range(3)]
    pieces, end1 = [], 0
    for num, (dims, rows) in enumerate(zip((((1, 2), 0), ((0, 1), 2), ((0, 2), 1)), share)):
        pieces.append(Piece(num, dims[0], dims[1], rows, end1))
        end1 += rows * PLANE
    rows1 = sum(share)
    rows2 = -(-n_slab * slab2 // (CUBE * 8)) * 8
    end2 = rows2 * CUBE

    def kernel(h0_hbm, aint_hbm, ahalo_hbm, idx_hbm, w0_hbm, w1_hbm, g_hbm,
               dw1_out, dw2_out, gf_out,
               h0, aint, ahalo, idx, w0, w1, g,
               pt, e1, z0, ft, e0,
               s0, halo0, o1, r1, sz, haloz, o0, r0,
               z0acc, d1acc, z1acc, gfacc,
               part1, part2, pair1_in, pair2_in, rs1_in, rs2_in, x_in, res1, res2,
               in_sem, fwd_sem, bwd_sem, zcp_sem, ocp_sem,
               pair1_sem, pair2_sem, rs1_sem, rs2_sem, x_r, ag1_r, ag2_r, back1_s, back2_s, early_s, gossip):
        me = lax.axis_index("nodes")
        core = lax.rem(me, 2)
        coord = (lax.rem(me // 2, SIDE), lax.rem(me // (2 * SIDE), SIDE), me // (2 * SIDE * SIDE))
        stride = (2, 2 * SIDE, 2 * SIDE * SIDE)
        mate = me + 1 - 2 * core

        def ring_steps(dim, c):
            d = lax.rem(coord[dim] + (SIDE - c), SIDE)
            return d * (SIDE - d) - d * (SIDE - d) // 3 * 2

        away = [[ring_steps(dim, c) for c in range(SIDE)] for dim in range(3)]

        def moved(dim, step):
            return lax.rem(coord[dim] + step, SIDE)

        def peer(steps):
            d = core
            for dim in range(3):
                d = d + moved(dim, steps[dim]) * stride[dim]
            return d

        def near(o):
            return lax.rem(me + (o + n_dev), n_dev)

        def signal(sem, d):
            pl.semaphore_signal(sem, inc=1, device_id={"nodes": d}, device_id_type=pl.DeviceIdType.MESH)

        def rcopy(src, dst, ss, rs, d):
            return pltpu.make_async_remote_copy(src_ref=src, dst_ref=dst, send_sem=ss, recv_sem=rs,
                                                device_id={"nodes": d}, device_id_type=pl.DeviceIdType.MESH)

        def lanes(ref, k):
            return ref.at[:, pl.ds(k * slots, slots)]

        def link_copies(src, dst, sems, sign):
            return [rcopy(lanes(src, k), lanes(dst, k), sems.at[0], sems.at[1 + k // 2], near(sign * OFFSETS[k])) for k in range(LINKS)]

        def link_wait(src, dst, sems, i):
            both = pl.ds(2 * i * slots, 2 * slots)
            rcopy(src.at[:, both], dst.at[:, both], sems.at[0], sems.at[1 + i], mate).wait_recv()

        def links_sent():
            for src, dst, sems in ((s0, halo0, fwd_sem), (o1, r1, bwd_sem), (sz, haloz, zcp_sem), (o0, r0, ocp_sem)):
                rcopy(src, dst, sems.at[0], sems.at[1], mate).wait_send()

        def start(copies):
            for cp in copies:
                cp.start()

        def wait(copies):
            for cp in copies:
                cp.wait()

        def on(which, name, *steps):
            @pl.when(core == which)
            def _():
                with jax.named_scope(name):
                    for step in steps:
                        step()

        barrier = pltpu.get_barrier_semaphore()
        ring = [peer(tuple(step if d == dim else 0 for d in range(3))) for dim in range(3) for step in (1, SIDE - 1)]
        greeted = [near(o) for o in OFFSETS] + [mate] + ring
        for d in greeted:
            signal(barrier, d)

        loads = [pltpu.make_async_copy(a, b, in_sem.at[i]) for i, (a, b) in enumerate((
            (idx_hbm, idx), (h0_hbm, h0), (g_hbm, g), (w1_hbm, w1), (ahalo_hbm, ahalo), (aint_hbm, aint), (w0_hbm, w0)))]
        start(loads)
        ld_idx, ld_h0, ld_g, ld_w1, ld_ahalo, ld_aint, ld_w0 = loads

        def gossip_send(i):
            for d in ring:
                signal(gossip.at[i % 2], d)

        def gossip_wait(i):
            pl.semaphore_wait(gossip.at[i % 2], len(ring))

        part1[...] = jnp.zeros_like(part1)
        part2[...] = jnp.zeros_like(part2)
        node_id = lax.broadcasted_iota(jnp.int32, (nodes, slots), 0)
        fwd = link_copies(s0, halo0, fwd_sem, 1)
        bwd = link_copies(o1, r1, bwd_sem, -1)
        zcp = link_copies(sz, haloz, zcp_sem, 1)
        ocp = link_copies(o0, r0, ocp_sem, -1)
        upper = pl.ds(2 * slots, 2 * slots)
        lower = pl.ds(0, 2 * slots)

        def select_rows(ks):
            for k in ks:
                pt[:, k * slots:(k + 1) * slots] = jnp.where(node_id == idx[k:k + 1, :], 1.0, 0.0).astype(BF16)

        with jax.named_scope("ld_idx"):
            ld_idx.wait()
        with jax.named_scope("pt"):
            select_rows((2, 3))
        with jax.named_scope("ld_h0"):
            ld_h0.wait()
        with jax.named_scope("s0"):
            s0[:, upper] = dot(h0[...], pt[:, upper], 1, 0).astype(BF16)
        with jax.named_scope("s0_low"):
            select_rows((0, 1))
            s0[:, lower] = dot(h0[...], pt[:, lower], 1, 0).astype(BF16)
        with jax.named_scope("barrier"):
            pl.semaphore_wait(barrier, len(greeted))
        with jax.named_scope("fwd_start"):
            start(fwd[2:] + fwd[:2])
            gossip_send(0)
        with jax.named_scope("e1"):
            ld_g.wait()
            ld_w1.wait()
            e1[...] = dot(w1[...], g[...], 0, 0).astype(BF16)
        with jax.named_scope("o1"):
            ld_ahalo.wait()
            o1[...] = dot(e1[...], ahalo[...], 1, 0).astype(BF16)
        on(0, "bwd_start0", lambda: start([bwd[2], bwd[0], bwd[1]]))
        on(1, "bwd_start1", lambda: start([bwd[3], bwd[1], bwd[0]]))
        with jax.named_scope("z0acc"):
            ld_aint.wait()
            z0acc[...] = dot(h0[...], aint[...], 1, 1)
        on(0, "bwd_rest0", bwd[3].start)
        on(1, "bwd_rest1", bwd[2].start)
        with jax.named_scope("gossip0"):
            gossip_wait(0)
            gossip_send(1)
        with jax.named_scope("d1acc"):
            d1acc[...] = dot(e1[...], aint[...], 1, 0)

        with jax.named_scope("fwd_wait_up"):
            link_wait(s0, halo0, fwd_sem, 1)
        with jax.named_scope("z0_up"):
            z0acc[...] = z0acc[...] + dot(halo0[:, upper], ahalo[:, upper], 1, 1)
        with jax.named_scope("fwd_wait_low"):
            link_wait(s0, halo0, fwd_sem, 0)
        with jax.named_scope("z0"):
            z0[...] = (z0acc[...] + dot(halo0[:, lower], ahalo[:, lower], 1, 1)).astype(BF16)
        halves = (zcp[:2], zcp[2:])
        for n in range(2):
            with jax.named_scope("sz%d" % n):
                cols = pl.ds(pl.multiple_of((core if n else 1 - core) * 2 * slots, 2 * slots), 2 * slots)
                sz[:, cols] = dot(z0[...], pt[:, cols], 1, 0).astype(BF16)
            on(0, "z_start%d" % n, lambda: start(halves[1 - n]))
            on(1, "z_start%d" % n, lambda: start(halves[n]))
        with jax.named_scope("gossip1"):
            gossip_wait(1)
            gossip_send(2)
        with jax.named_scope("h1"):
            ld_w0.wait()
            ft[...] = jnp.maximum(dot(w0[...], z0[...], 0, 0), 0.0).astype(BF16)
        with jax.named_scope("z1acc"):
            z1acc[...] = dot(ft[...], aint[...], 1, 1)
        with jax.named_scope("gossip2"):
            gossip_wait(2)
            gossip_send(3)

        with jax.named_scope("bwd_wait_up"):
            link_wait(o1, r1, bwd_sem, 1)
        with jax.named_scope("d1_up"):
            d1acc[...] = d1acc[...] + dot(r1[:, upper], pt[:, upper], 1, 1)
        with jax.named_scope("bwd_wait_low"):
            link_wait(o1, r1, bwd_sem, 0)

        def first_half(h):
            rows = pl.ds(pl.multiple_of(h * half_hid, half_hid), half_hid)
            d1 = d1acc[rows, :] + dot(r1[rows, lower], pt[:, lower], 1, 1)
            ft[rows, :] = jnp.where(ft[rows, :] > 0, d1, 0.0).astype(BF16)
            dw1 = dot(z0[...], ft[rows, :], 1, 1)
            for s in range(half_hid // 128):
                part1[h, pl.ds(s * slab1, feat), :] = dw1[:, s * 128:(s + 1) * 128]

        def rows_of(ref, n, i):
            return ref.at[pl.ds(pl.multiple_of(i * n, 8), n), :]

        def rows_wait(ref, rows, ss, rs):
            some = ref.at[pl.ds(0, rows), :]
            if ss is not None:
                rcopy(some, some, ss, ss, mate).wait_send()
            if rs is not None:
                rcopy(some, some, rs, rs, mate).wait_recv()

        pair1 = rcopy(part1.at[1 - core, pl.ds(0, half_rows), :], pair1_in, pair1_sem.at[0], pair1_sem.at[1], mate)

        def plane_id(p, ab=(0, 0)):
            return moved(p.plane[0], ab[0]) * SIDE + moved(p.plane[1], ab[1])

        def chunk1(ref, p, i):
            return ref.at[core, pl.ds(pl.multiple_of(p.base + i * p.rows, 8), p.rows), :]

        def stage(ref, p, i):
            return ref.at[p.num, i, pl.ds(0, p.rows), :]

        def rs1_send(group):
            start([rcopy(chunk1(part1, p, plane_id(p, ab)), stage(rs1_in, p, plane_id(p)), rs1_sem.at[0], rs1_sem.at[1], peer(p.steps(ab)))
                   for ab in PLANE_PEERS for p in group])
            for p in group:
                rs1_in[p.num, plane_id(p), pl.ds(0, p.rows), :] = part1[core, pl.ds(pl.multiple_of(p.base + plane_id(p) * p.rows, 8), p.rows), :]

        def rs1_start():
            used = pl.ds(0, half_rows)
            part1[core, used, :] = part1[core, used, :] + pair1_in[...]
            rs1_send(pieces)

        def rs1_finish():
            rows_wait(part1.at[0], (PLANE - 1) * rows1, rs1_sem.at[0], rs1_sem.at[1])
            for p in pieces:
                total = rs1_in[p.num, 0, 0:p.rows, :]
                for i in range(1, PLANE):
                    total = total + rs1_in[p.num, i, 0:p.rows, :]
                x_in[p.num, coord[p.cross], pl.ds(0, p.rows), :] = total
            start([rcopy(stage(x_in, p, coord[p.cross]), stage(x_in, p, coord[p.cross]), rs1_sem.at[0], x_r, peer(p.across(step)))
                   for step in (2, 1, 3) for p in pieces])

        def x1_finish():
            rows_wait(part1.at[0], (SIDE - 1) * rows1, rs1_sem.at[0], x_r)
            for p in pieces:
                total = x_in[p.num, 0, 0:p.rows, :]
                for i in range(1, SIDE):
                    total = total + x_in[p.num, i, 0:p.rows, :]
                res1[core, pl.ds(pl.multiple_of(p.base + plane_id(p) * p.rows, 8), p.rows), :] = total
            mine = [chunk1(res1, p, plane_id(p)) for p in pieces]
            order = [release_order(p.plane) for p in pieces]
            for spots in zip(*order):
                for p, ref, (a, b) in zip(pieces, mine, spots):
                    steps = away[p.plane[0]][a] + away[p.plane[1]][b]
                    d = core + a * stride[p.plane[0]] + b * stride[p.plane[1]] + coord[p.cross] * stride[p.cross]
                    rcopy(ref, ref, rs1_sem.at[0], ag1_r.at[steps], d + jnp.where(steps == 0, mate - me, 0)).start()

        def back1(p, i):
            return rcopy(chunk1(res1, p, i), chunk1(res1, p, i), back1_s, ag1_r.at[0], mate)

        def ag1_step(n):
            near_n = [ab for ab in PLANE_PEERS if hops(ab) == n]
            rows_wait(part1.at[0], len(near_n) * rows1, None, ag1_r.at[n])
            start([back1(p, plane_id(p, ab)) for ab in near_n for p in pieces])

        def back1_finish():
            rows_wait(part1.at[0], PLANE * rows1, None, ag1_r.at[0])

        def back1_sent():
            rows_wait(part1.at[0], PLANE * rows1, rs1_sem.at[0], None)
            rows_wait(part1.at[0], (PLANE - 1) * rows1, back1_s, None)

        my_cube = coord[0] + SIDE * (coord[1] + SIDE * coord[2])
        pair2 = rcopy(part2.at[pl.ds(0, n_slab * slab2), :], pair2_in, pair2_sem.at[0], pair2_sem.at[1], mate)

        def cube_id(steps):
            return moved(0, steps[0]) + SIDE * (moved(1, steps[1]) + SIDE * moved(2, steps[2]))

        def rs2_start():
            pair2.wait_recv()
            used = pl.ds(0, n_slab * slab2)
            part2[used, :] = part2[used, :] + pair2_in[...]
            start([rcopy(rows_of(part2, rows2, cube_id(st)), rs2_in.at[my_cube], rs2_sem.at[0], rs2_sem.at[1], peer(st)) for st in CUBE_PEERS])
            rs2_in[my_cube] = part2[pl.ds(pl.multiple_of(my_cube * rows2, 8), rows2), :]

        def rs2_finish():
            rows_wait(part2, (CUBE - 1) * rows2, rs2_sem.at[0], rs2_sem.at[1])
            sums = [rs2_in[i] for i in range(CUBE)]
            while len(sums) > 1:
                sums = [a + b for a, b in zip(sums[::2], sums[1::2])]
            res2[pl.ds(pl.multiple_of(my_cube * rows2, 8), rows2), :] = sums[0]
            mine = rows_of(res2, rows2, my_cube)
            for a, b, c in release_order((0, 1, 2)):
                steps = away[0][a] + away[1][b] + away[2][c]
                d = core + a * stride[0] + b * stride[1] + c * stride[2]
                rcopy(mine, mine, rs2_sem.at[0], ag2_r.at[steps], d + jnp.where(steps == 0, mate - me, 0)).start()
                if (a, b, c) == (0, 0, 0):
                    pl.when(me != 1)(rcopy(mine, mine, early_s, ag2_r.at[0], 0).start)

        def back2(i):
            return rcopy(rows_of(res2, rows2, i), rows_of(res2, rows2, i), back2_s, ag2_r.at[0], mate)

        def ag2_step(n):
            near_n = [st for st in CUBE_PEERS if hops(st) == n]
            rows_wait(part2, len(near_n) * rows2, None, ag2_r.at[n])
            pl.when(me != 1)(lambda: start([back2(cube_id(st)) for st in near_n]))

        def ag2_finish():
            rows_wait(part2, CUBE * rows2, rs2_sem.at[0], None)

            @pl.when(me != 1)
            def _():
                rows_wait(part2, (CUBE - 1) * rows2, back2_s, None)
                rows_wait(part2, rows2, early_s, None)

        def run(name, *steps):
            with jax.named_scope(name):
                for step in steps:
                    step()

        run("half_mate", lambda: first_half(1 - core))
        run("pair1_start", pair1.start)
        run("half_own", lambda: first_half(core))
        with jax.named_scope("e0"):
            e0[...] = dot(w0[...], ft[...], 1, 0).astype(BF16)
        with jax.named_scope("gossip3"):
            gossip_wait(3)
            gossip_send(4)
        run("pair1_wait", pair1.wait)
        run("rs1_start", rs1_start)

        def z1_half(n):
            cols = pl.ds(pl.multiple_of((core if n else 1 - core) * 2 * slots, 2 * slots), 2 * slots)
            on(0, "z_wait%d" % n, lambda: link_wait(sz, haloz, zcp_sem, 1 - n))
            on(1, "z_wait%d" % n, lambda: link_wait(sz, haloz, zcp_sem, n))
            with jax.named_scope("z1_%d" % n):
                h1h = jnp.maximum(dot(w0[...], haloz[:, cols], 0, 0), 0.0).astype(BF16)
                return z1acc[...] + dot(h1h, ahalo[:, cols], 1, 1)

        z1acc[...] = z1_half(0)
        z1 = z1_half(1).astype(BF16)
        with jax.named_scope("dw2"):
            dw2 = dot(g[...], z1, 1, 1)
            for s in range(n_slab):
                part2[pl.ds(s * slab2, cls), :] = dw2[:, s * 128:(s + 1) * 128]
        on(0, "pair2_start", pair2.start)
        with jax.named_scope("gossip4"):
            gossip_wait(4)
        with jax.named_scope("o0"):
            o0[...] = dot(e0[...], ahalo[...], 1, 0).astype(BF16)
        with jax.named_scope("gfacc"):
            gfacc[...] = dot(e0[...], aint[...], 1, 0)
        on(1, "rs2_start", rs2_start)
        run("rs1_finish", rs1_finish)
        with jax.named_scope("o_start"):
            start(ocp)
        run("x1_finish", x1_finish)
        on(1, "rs2_finish", rs2_finish)
        with jax.named_scope("o_wait"):
            link_wait(o0, r0, ocp_sem, 0)
            link_wait(o0, r0, ocp_sem, 1)
        with jax.named_scope("gf"):
            gf_out[...] = gfacc[...] + dot(r0[...], pt[...], 1, 1)
        for n in range(1, 7):
            if n <= 4:
                run("ag1_%d" % n, lambda: ag1_step(n))
            on(1, "ag2_%d" % n, lambda: ag2_step(n))
        run("back1_finish", back1_finish)
        on(0, "back2_wait", lambda: rows_wait(part2, CUBE * rows2, None, ag2_r.at[0]), pair2.wait_send)
        with jax.named_scope("outs"):
            for s in range(n_slab):
                h, q = s // (n_slab // 2), s % (n_slab // 2)
                dw1_out[:, s * 128:(s + 1) * 128] = res1[h, pl.ds(q * slab1, feat), :]
                dw2_out[:, s * 128:(s + 1) * 128] = res2[pl.ds(s * slab2, cls), :]

        run("links_sent", links_sent)
        run("back1_sent", back1_sent)
        on(1, "ag2_finish", ag2_finish)

    V = pltpu.VMEM
    D = pltpu.SemaphoreType.DMA
    link_sems = [D((3,))] * 4
    scratch = [
        V((feat, nodes), BF16), V((nodes, nodes), BF16), V((nodes, all_slots), BF16), V((LINKS, slots), jnp.int32),
        V((feat, hid), BF16), V((cls, hid), BF16), V((cls, nodes), BF16),
        V((nodes, all_slots), BF16), V((hid, nodes), BF16), V((feat, nodes), BF16), V((hid, nodes), BF16), V((feat, nodes), BF16),
        V((feat, all_slots), BF16), V((feat, all_slots), BF16), V((hid, all_slots), BF16), V((hid, all_slots), BF16),
        V((feat, all_slots), BF16), V((feat, all_slots), BF16), V((feat, all_slots), BF16), V((feat, all_slots), BF16),
        V((feat, nodes), F32), V((hid, nodes), F32), V((hid, nodes), F32), V((feat, nodes), F32),
        V((2, end1, 128), F32), V((end2, 128), F32), V((half_rows, 128), F32), V((n_slab * slab2, 128), F32),
        V((3, PLANE, max(share), 128), F32), V((CUBE, rows2, 128), F32), V((3, SIDE, max(share), 128), F32), V((2, end1, 128), F32), V((end2, 128), F32),
        D((7,)), *link_sems, D((2,)), D((2,)), D((2,)), D((2,)), D, D((5,)), D((7,)), D, D, D, pltpu.SemaphoreType.REGULAR((2,)),
    ]
    out_bytes = 4 * (slab1 * hid + slab2 * hid + slab1 * nodes)
    any_spec = pl.BlockSpec(memory_space=pl.ANY)
    vmem_spec = pl.BlockSpec(memory_space=pltpu.VMEM)
    return pl.pallas_call(
        kernel,
        out_shape=(pltpu.VMEM((feat, hid), F32), pltpu.VMEM((cls, hid), F32), pltpu.VMEM((feat, nodes), F32)),
        in_specs=[any_spec] * 7,
        out_specs=(vmem_spec, vmem_spec, vmem_spec),
        scratch_shapes=scratch,
        compiler_params=pltpu.CompilerParams(collective_id=0, has_side_effects=True, vmem_limit_bytes=VMEM_BYTES - out_bytes - 65536),
        name="gcn_backward",
    )


def write_out(feat, hid, cls, nodes):
    def kernel(dw1, dw2, gf, dw1_out, dw2_out, gf_out, sems):
        pairs = [(dw1, dw1_out), (dw2, dw2_out)]
        for i in range(WRITES):
            cols = pl.ds(i * (nodes // WRITES), nodes // WRITES)
            pairs.append((gf.at[:, cols], gf_out.at[:, cols]))
        copies = [pltpu.make_async_copy(a, b, sems.at[i]) for i, (a, b) in enumerate(pairs)]
        for cp in copies:
            cp.start()
        for cp in copies:
            cp.wait()

    return pl.pallas_call(
        kernel,
        out_shape=(jax.ShapeDtypeStruct((feat, hid), F32), jax.ShapeDtypeStruct((cls, hid), F32), jax.ShapeDtypeStruct((feat, nodes), F32)),
        in_specs=[pl.BlockSpec(memory_space=pltpu.VMEM)] * 3,
        out_specs=(pl.BlockSpec(memory_space=pl.ANY),) * 3,
        scratch_shapes=[pltpu.SemaphoreType.DMA((2 + WRITES,))],
        compiler_params=pltpu.CompilerParams(vmem_limit_bytes=4 * 1024 * 1024),
        name="write_out",
    )


def solution(mesh):
    axis_size = mesh.shape["nodes"]
    row_spec = P(("graph", "nodes"), None)
    replicated = P(None, None)
    part_spec = P("graph", None)

    def device_step(node_feats, a_int, a_halo, send_idx, w_first, w_second, grad_out):
        nodes, feat = node_feats.shape
        hid, cls = w_second.shape
        call = build(axis_size, nodes, feat, hid, cls, send_idx.shape[1])
        dw1, dw2, gf = call(node_feats.T, a_int, a_halo, send_idx, w_first, w_second.T, grad_out.T)
        dw1, dw2, gf = write_out(feat, hid, cls, nodes)(dw1, dw2, gf)
        return dw1, dw2.T, gf.T

    return jax.shard_map(device_step, mesh=mesh, in_specs=(row_spec, row_spec, row_spec, row_spec, replicated, replicated, row_spec), out_specs=(part_spec, part_spec, row_spec), check_vma=False)
```

```python
import jax
import jax.numpy as jnp
from jax import lax
from jax.experimental import pallas as pl
from jax.experimental.pallas import tpu as pltpu
from jax.sharding import PartitionSpec as P

F32 = jnp.float32
BF16 = jnp.bfloat16
SIDE = 4
PLANE = SIDE * SIDE
CUBE = PLANE * SIDE
OFFSETS = (1, -1, 2, -2)
LINKS = 4
VMEM_BYTES = 67043328
WRITES = 4


def dot(a, b, ca, cb):
    return lax.dot_general(a, b, (((ca,), (cb,)), ((), ())), preferred_element_type=F32)


def hops(step):
    return sum(min(d, SIDE - d) for d in step)


PLANE_PEERS = sorted(((a, b) for a in range(SIDE) for b in range(SIDE) if a or b), key=hops, reverse=True)
CUBE_PEERS = sorted(((a, b, c) for a in range(SIDE) for b in range(SIDE) for c in range(SIDE) if a or b or c), key=hops, reverse=True)


RELEASE = ((0.0, 0.5, 0.9, 1.1), (0.0, 0.6, 1.2, 1.4), (0.0, 0.9, 1.8, 2.4))


def release_order(dims):
    spots = [()]
    for _ in dims:
        spots = [s + (c,) for s in spots for c in range(SIDE)]
    return sorted(spots, key=lambda s: sum(RELEASE[d][c] for d, c in zip(dims, s)))


class Piece:
    def __init__(self, num, plane, cross, rows, base):
        self.num, self.plane, self.cross, self.rows, self.base = num, plane, cross, rows, base

    def steps(self, ab):
        st = [0, 0, 0]
        st[self.plane[0]], st[self.plane[1]] = ab
        return tuple(st)

    def across(self, step):
        st = [0, 0, 0]
        st[self.cross] = step
        return tuple(st)


def build(n_dev, nodes, feat, hid, cls, slots):
    all_slots = LINKS * slots
    half_hid = hid // 2
    n_slab = hid // 128
    slab1 = (feat + 7) // 8 * 8
    slab2 = (cls + 7) // 8 * 8
    half_rows = n_slab // 2 * slab1
    units = -(-half_rows // (PLANE * 8))
    share = [8 * ((units + 2 - p) // 3) for p in range(3)]
    pieces, end1 = [], 0
    for num, (dims, rows) in enumerate(zip((((1, 2), 0), ((0, 1), 2), ((0, 2), 1)), share)):
        pieces.append(Piece(num, dims[0], dims[1], rows, end1))
        end1 += rows * PLANE
    rows1 = sum(share)
    rows2 = -(-n_slab * slab2 // (CUBE * 8)) * 8
    end2 = rows2 * CUBE

    def kernel(h0_hbm, aint_hbm, ahalo_hbm, idx_hbm, w0_hbm, w1_hbm, g_hbm,
               dw1_out, dw2_out, gf_out,
               h0, aint, ahalo, idx, w0, w1, g,
               pt, e1, z0, ft, e0,
               s0, halo0, o1, r1, sz, haloz, o0, r0,
               z0acc, d1acc, z1acc, gfacc,
               part1, part2, pair1_in, pair2_in, rs1_in, rs2_in, x_in, res1, res2,
               in_sem, fwd_sem, bwd_sem, zcp_sem, ocp_sem,
               pair1_sem, pair2_sem, rs1_sem, rs1_r, rs2_sem, x_s, x_r, ag1_r, ag2_r, back1_s, back2_s, early_s, gossip):
        me = lax.axis_index("nodes")
        core = lax.rem(me, 2)
        coord = (lax.rem(me // 2, SIDE), lax.rem(me // (2 * SIDE), SIDE), me // (2 * SIDE * SIDE))
        stride = (2, 2 * SIDE, 2 * SIDE * SIDE)
        mate = me + 1 - 2 * core

        def ring_steps(dim, c):
            d = lax.rem(coord[dim] + (SIDE - c), SIDE)
            return d * (SIDE - d) - d * (SIDE - d) // 3 * 2

        away = [[ring_steps(dim, c) for c in range(SIDE)] for dim in range(3)]

        def moved(dim, step):
            return lax.rem(coord[dim] + step, SIDE)

        def peer(steps):
            d = core
            for dim in range(3):
                d = d + moved(dim, steps[dim]) * stride[dim]
            return d

        def near(o):
            return lax.rem(me + (o + n_dev), n_dev)

        def signal(sem, d):
            pl.semaphore_signal(sem, inc=1, device_id={"nodes": d}, device_id_type=pl.DeviceIdType.MESH)

        def rcopy(src, dst, ss, rs, d):
            return pltpu.make_async_remote_copy(src_ref=src, dst_ref=dst, send_sem=ss, recv_sem=rs,
                                                device_id={"nodes": d}, device_id_type=pl.DeviceIdType.MESH)

        def lanes(ref, k):
            return ref.at[:, pl.ds(k * slots, slots)]

        def link_copies(src, dst, sems, sign):
            return [rcopy(lanes(src, k), lanes(dst, k), sems.at[0], sems.at[1 + k // 2], near(sign * OFFSETS[k])) for k in range(LINKS)]

        def link_wait(src, dst, sems, i):
            both = pl.ds(2 * i * slots, 2 * slots)
            rcopy(src.at[:, both], dst.at[:, both], sems.at[0], sems.at[1 + i], mate).wait_recv()

        def links_sent():
            for src, dst, sems in ((s0, halo0, fwd_sem), (o1, r1, bwd_sem), (sz, haloz, zcp_sem), (o0, r0, ocp_sem)):
                rcopy(src, dst, sems.at[0], sems.at[1], mate).wait_send()

        def start(copies):
            for cp in copies:
                cp.start()

        def wait(copies):
            for cp in copies:
                cp.wait()

        def on(which, name, *steps):
            @pl.when(core == which)
            def _():
                with jax.named_scope(name):
                    for step in steps:
                        step()

        barrier = pltpu.get_barrier_semaphore()
        ring = [peer(tuple(step if d == dim else 0 for d in range(3))) for dim in range(3) for step in (1, SIDE - 1)]
        greeted = [near(o) for o in OFFSETS] + [mate] + ring
        for d in greeted:
            signal(barrier, d)

        loads = [pltpu.make_async_copy(a, b, in_sem.at[i]) for i, (a, b) in enumerate((
            (idx_hbm, idx), (h0_hbm, h0), (g_hbm, g), (w1_hbm, w1), (ahalo_hbm, ahalo), (aint_hbm, aint), (w0_hbm, w0)))]
        start(loads)
        ld_idx, ld_h0, ld_g, ld_w1, ld_ahalo, ld_aint, ld_w0 = loads

        def gossip_send(i):
            for d in ring:
                signal(gossip.at[i % 2], d)

        def gossip_wait(i):
            pl.semaphore_wait(gossip.at[i % 2], len(ring))

        part1[...] = jnp.zeros_like(part1)
        part2[...] = jnp.zeros_like(part2)
        node_id = lax.broadcasted_iota(jnp.int32, (nodes, slots), 0)
        fwd = link_copies(s0, halo0, fwd_sem, 1)
        bwd = link_copies(o1, r1, bwd_sem, -1)
        zcp = link_copies(sz, haloz, zcp_sem, 1)
        ocp = link_copies(o0, r0, ocp_sem, -1)
        upper = pl.ds(2 * slots, 2 * slots)
        lower = pl.ds(0, 2 * slots)

        def select_rows(ks):
            for k in ks:
                pt[:, k * slots:(k + 1) * slots] = jnp.where(node_id == idx[k:k + 1, :], 1.0, 0.0).astype(BF16)

        with jax.named_scope("ld_idx"):
            ld_idx.wait()
        with jax.named_scope("pt"):
            select_rows((2, 3))
        with jax.named_scope("ld_h0"):
            ld_h0.wait()
        with jax.named_scope("s0"):
            s0[:, upper] = dot(h0[...], pt[:, upper], 1, 0).astype(BF16)
        with jax.named_scope("s0_low"):
            select_rows((0, 1))
            s0[:, lower] = dot(h0[...], pt[:, lower], 1, 0).astype(BF16)
        with jax.named_scope("barrier"):
            pl.semaphore_wait(barrier, len(greeted))
        with jax.named_scope("fwd_start"):
            start(fwd[2:] + fwd[:2])
            gossip_send(0)
        with jax.named_scope("e1"):
            ld_g.wait()
            ld_w1.wait()
            e1[...] = dot(w1[...], g[...], 0, 0).astype(BF16)
        with jax.named_scope("o1"):
            ld_ahalo.wait()
            o1[...] = dot(e1[...], ahalo[...], 1, 0).astype(BF16)
        on(0, "bwd_start0", lambda: start([bwd[2], bwd[0], bwd[1]]))
        on(1, "bwd_start1", lambda: start([bwd[3], bwd[1], bwd[0]]))
        with jax.named_scope("z0acc"):
            ld_aint.wait()
            z0acc[...] = dot(h0[...], aint[...], 1, 1)
        on(0, "bwd_rest0", bwd[3].start)
        on(1, "bwd_rest1", bwd[2].start)
        with jax.named_scope("gossip0"):
            gossip_wait(0)
            gossip_send(1)
        with jax.named_scope("d1acc"):
            d1acc[...] = dot(e1[...], aint[...], 1, 0)

        with jax.named_scope("fwd_wait_up"):
            link_wait(s0, halo0, fwd_sem, 1)
        with jax.named_scope("z0_up"):
            z0acc[...] = z0acc[...] + dot(halo0[:, upper], ahalo[:, upper], 1, 1)
        with jax.named_scope("fwd_wait_low"):
            link_wait(s0, halo0, fwd_sem, 0)
        with jax.named_scope("z0"):
            z0[...] = (z0acc[...] + dot(halo0[:, lower], ahalo[:, lower], 1, 1)).astype(BF16)
        halves = (zcp[:2], zcp[2:])
        for n in range(2):
            with jax.named_scope("sz%d" % n):
                cols = pl.ds(pl.multiple_of((core if n else 1 - core) * 2 * slots, 2 * slots), 2 * slots)
                sz[:, cols] = dot(z0[...], pt[:, cols], 1, 0).astype(BF16)
            on(0, "z_start%d" % n, lambda: start(halves[1 - n]))
            on(1, "z_start%d" % n, lambda: start(halves[n]))
        with jax.named_scope("gossip1"):
            gossip_wait(1)
            gossip_send(2)
        with jax.named_scope("h1"):
            ld_w0.wait()
            ft[...] = jnp.maximum(dot(w0[...], z0[...], 0, 0), 0.0).astype(BF16)
        with jax.named_scope("z1acc"):
            z1acc[...] = dot(ft[...], aint[...], 1, 1)
        with jax.named_scope("gossip2"):
            gossip_wait(2)
            gossip_send(3)

        with jax.named_scope("bwd_wait_up"):
            link_wait(o1, r1, bwd_sem, 1)
        with jax.named_scope("d1_up"):
            d1acc[...] = d1acc[...] + dot(r1[:, upper], pt[:, upper], 1, 1)
        with jax.named_scope("bwd_wait_low"):
            link_wait(o1, r1, bwd_sem, 0)

        def first_half(h):
            rows = pl.ds(pl.multiple_of(h * half_hid, half_hid), half_hid)
            d1 = d1acc[rows, :] + dot(r1[rows, lower], pt[:, lower], 1, 1)
            ft[rows, :] = jnp.where(ft[rows, :] > 0, d1, 0.0).astype(BF16)
            dw1 = dot(z0[...], ft[rows, :], 1, 1)
            for s in range(half_hid // 128):
                part1[h, pl.ds(s * slab1, feat), :] = dw1[:, s * 128:(s + 1) * 128]

        def rows_of(ref, n, i):
            return ref.at[pl.ds(pl.multiple_of(i * n, 8), n), :]

        def rows_wait(ref, rows, ss, rs):
            some = ref.at[pl.ds(0, rows), :]
            if ss is not None:
                rcopy(some, some, ss, ss, mate).wait_send()
            if rs is not None:
                rcopy(some, some, rs, rs, mate).wait_recv()

        pair1 = rcopy(part1.at[1 - core, pl.ds(0, half_rows), :], pair1_in, pair1_sem.at[0], pair1_sem.at[1], mate)

        def plane_id(p, ab=(0, 0)):
            return moved(p.plane[0], ab[0]) * SIDE + moved(p.plane[1], ab[1])

        def chunk1(ref, p, i):
            return ref.at[core, pl.ds(pl.multiple_of(p.base + i * p.rows, 8), p.rows), :]

        def stage(ref, p, i):
            return ref.at[p.num, i, pl.ds(0, p.rows), :]

        def rs1_send(group):
            start([rcopy(chunk1(part1, p, plane_id(p, ab)), stage(rs1_in, p, plane_id(p)), rs1_sem.at[0], rs1_r.at[p.num], peer(p.steps(ab)))
                   for ab in PLANE_PEERS for p in group])
            for p in group:
                rs1_in[p.num, plane_id(p), pl.ds(0, p.rows), :] = part1[core, pl.ds(pl.multiple_of(p.base + plane_id(p) * p.rows, 8), p.rows), :]

        def rs1_start():
            used = pl.ds(0, half_rows)
            part1[core, used, :] = part1[core, used, :] + pair1_in[...]
            rs1_send(pieces)

        def rs1_finish():
            for p in pieces:
                rows_wait(part1.at[0], (PLANE - 1) * p.rows, None, rs1_r.at[p.num])
                total = rs1_in[p.num, 0, 0:p.rows, :]
                for i in range(1, PLANE):
                    total = total + rs1_in[p.num, i, 0:p.rows, :]
                mine = stage(x_in, p, coord[p.cross])
                x_in[p.num, coord[p.cross], pl.ds(0, p.rows), :] = total
                start([rcopy(mine, mine, x_s, x_r.at[p.num], peer(p.across(step))) for step in (2, 1, 3)])
            rows_wait(part1.at[0], (PLANE - 1) * rows1, rs1_sem.at[0], None)

        def x1_finish():
            for p in pieces:
                rows_wait(part1.at[0], (SIDE - 1) * p.rows, None, x_r.at[p.num])
                total = x_in[p.num, 0, 0:p.rows, :]
                for i in range(1, SIDE):
                    total = total + x_in[p.num, i, 0:p.rows, :]
                res1[core, pl.ds(pl.multiple_of(p.base + plane_id(p) * p.rows, 8), p.rows), :] = total
                mine = chunk1(res1, p, plane_id(p))
                for a, b in release_order(p.plane):
                    steps = away[p.plane[0]][a] + away[p.plane[1]][b]
                    d = core + a * stride[p.plane[0]] + b * stride[p.plane[1]] + coord[p.cross] * stride[p.cross]
                    rcopy(mine, mine, rs1_sem.at[0], ag1_r.at[steps], d + jnp.where(steps == 0, mate - me, 0)).start()
            rows_wait(part1.at[0], (SIDE - 1) * rows1, x_s, None)

        def back1(p, i):
            return rcopy(chunk1(res1, p, i), chunk1(res1, p, i), back1_s, ag1_r.at[0], mate)

        def ag1_step(n):
            near_n = [ab for ab in PLANE_PEERS if hops(ab) == n]
            rows_wait(part1.at[0], len(near_n) * rows1, None, ag1_r.at[n])
            start([back1(p, plane_id(p, ab)) for ab in near_n for p in pieces])

        def back1_finish():
            rows_wait(part1.at[0], PLANE * rows1, None, ag1_r.at[0])

        def back1_sent():
            rows_wait(part1.at[0], PLANE * rows1, rs1_sem.at[0], None)
            rows_wait(part1.at[0], (PLANE - 1) * rows1, back1_s, None)

        my_cube = coord[0] + SIDE * (coord[1] + SIDE * coord[2])
        pair2 = rcopy(part2.at[pl.ds(0, n_slab * slab2), :], pair2_in, pair2_sem.at[0], pair2_sem.at[1], mate)

        def cube_id(steps):
            return moved(0, steps[0]) + SIDE * (moved(1, steps[1]) + SIDE * moved(2, steps[2]))

        def rs2_start():
            pair2.wait_recv()
            used = pl.ds(0, n_slab * slab2)
            part2[used, :] = part2[used, :] + pair2_in[...]
            start([rcopy(rows_of(part2, rows2, cube_id(st)), rs2_in.at[my_cube], rs2_sem.at[0], rs2_sem.at[1], peer(st)) for st in CUBE_PEERS])
            rs2_in[my_cube] = part2[pl.ds(pl.multiple_of(my_cube * rows2, 8), rows2), :]

        def rs2_finish():
            rows_wait(part2, (CUBE - 1) * rows2, rs2_sem.at[0], rs2_sem.at[1])
            sums = [rs2_in[i] for i in range(CUBE)]
            while len(sums) > 1:
                sums = [a + b for a, b in zip(sums[::2], sums[1::2])]
            res2[pl.ds(pl.multiple_of(my_cube * rows2, 8), rows2), :] = sums[0]
            mine = rows_of(res2, rows2, my_cube)
            for a, b, c in release_order((0, 1, 2)):
                steps = away[0][a] + away[1][b] + away[2][c]
                d = core + a * stride[0] + b * stride[1] + c * stride[2]
                rcopy(mine, mine, rs2_sem.at[0], ag2_r.at[steps], d + jnp.where(steps == 0, mate - me, 0)).start()
                if (a, b, c) == (0, 0, 0):
                    pl.when(me != 1)(rcopy(mine, mine, early_s, ag2_r.at[0], 0).start)

        def back2(i):
            return rcopy(rows_of(res2, rows2, i), rows_of(res2, rows2, i), back2_s, ag2_r.at[0], mate)

        def ag2_step(n):
            near_n = [st for st in CUBE_PEERS if hops(st) == n]
            rows_wait(part2, len(near_n) * rows2, None, ag2_r.at[n])
            pl.when(me != 1)(lambda: start([back2(cube_id(st)) for st in near_n]))

        def ag2_finish():
            rows_wait(part2, CUBE * rows2, rs2_sem.at[0], None)

            @pl.when(me != 1)
            def _():
                rows_wait(part2, (CUBE - 1) * rows2, back2_s, None)
                rows_wait(part2, rows2, early_s, None)

        def run(name, *steps):
            with jax.named_scope(name):
                for step in steps:
                    step()

        run("half_mate", lambda: first_half(1 - core))
        run("pair1_start", pair1.start)
        run("half_own", lambda: first_half(core))
        with jax.named_scope("e0"):
            e0[...] = dot(w0[...], ft[...], 1, 0).astype(BF16)
        with jax.named_scope("gossip3"):
            gossip_wait(3)
            gossip_send(4)
        run("pair1_wait", pair1.wait)
        run("rs1_start", rs1_start)

        def z1_half(n):
            cols = pl.ds(pl.multiple_of((core if n else 1 - core) * 2 * slots, 2 * slots), 2 * slots)
            on(0, "z_wait%d" % n, lambda: link_wait(sz, haloz, zcp_sem, 1 - n))
            on(1, "z_wait%d" % n, lambda: link_wait(sz, haloz, zcp_sem, n))
            with jax.named_scope("z1_%d" % n):
                h1h = jnp.maximum(dot(w0[...], haloz[:, cols], 0, 0), 0.0).astype(BF16)
                return z1acc[...] + dot(h1h, ahalo[:, cols], 1, 1)

        z1acc[...] = z1_half(0)
        z1 = z1_half(1).astype(BF16)
        with jax.named_scope("dw2"):
            dw2 = dot(g[...], z1, 1, 1)
            for s in range(n_slab):
                part2[pl.ds(s * slab2, cls), :] = dw2[:, s * 128:(s + 1) * 128]
        on(0, "pair2_start", pair2.start)
        with jax.named_scope("gossip4"):
            gossip_wait(4)
        with jax.named_scope("o0"):
            o0[...] = dot(e0[...], ahalo[...], 1, 0).astype(BF16)
            pl.when(me == n_dev - 1)(ocp[3].start)
        with jax.named_scope("gfacc"):
            gfacc[...] = dot(e0[...], aint[...], 1, 0)
        on(1, "rs2_start", rs2_start)
        run("rs1_finish", rs1_finish)
        with jax.named_scope("o_start"):
            start(ocp[:3])
            pl.when(me < n_dev - 1)(ocp[3].start)
        run("x1_finish", x1_finish)
        on(1, "rs2_finish", rs2_finish)
        with jax.named_scope("o_wait"):
            link_wait(o0, r0, ocp_sem, 0)
            link_wait(o0, r0, ocp_sem, 1)
        with jax.named_scope("gf"):
            gf_out[...] = gfacc[...] + dot(r0[...], pt[...], 1, 1)
        for n in range(1, 7):
            if n <= 4:
                run("ag1_%d" % n, lambda: ag1_step(n))
            on(1, "ag2_%d" % n, lambda: ag2_step(n))
        run("back1_finish", back1_finish)
        on(0, "back2_wait", lambda: rows_wait(part2, CUBE * rows2, None, ag2_r.at[0]), pair2.wait_send)
        with jax.named_scope("outs"):
            for s in range(n_slab):
                h, q = s // (n_slab // 2), s % (n_slab // 2)
                dw1_out[:, s * 128:(s + 1) * 128] = res1[h, pl.ds(q * slab1, feat), :]
                dw2_out[:, s * 128:(s + 1) * 128] = res2[pl.ds(s * slab2, cls), :]

        run("links_sent", links_sent)
        run("back1_sent", back1_sent)
        on(1, "ag2_finish", ag2_finish)

    V = pltpu.VMEM
    D = pltpu.SemaphoreType.DMA
    link_sems = [D((3,))] * 4
    scratch = [
        V((feat, nodes), BF16), V((nodes, nodes), BF16), V((nodes, all_slots), BF16), V((LINKS, slots), jnp.int32),
        V((feat, hid), BF16), V((cls, hid), BF16), V((cls, nodes), BF16),
        V((nodes, all_slots), BF16), V((hid, nodes), BF16), V((feat, nodes), BF16), V((hid, nodes), BF16), V((feat, nodes), BF16),
        V((feat, all_slots), BF16), V((feat, all_slots), BF16), V((hid, all_slots), BF16), V((hid, all_slots), BF16),
        V((feat, all_slots), BF16), V((feat, all_slots), BF16), V((feat, all_slots), BF16), V((feat, all_slots), BF16),
        V((feat, nodes), F32), V((hid, nodes), F32), V((hid, nodes), F32), V((feat, nodes), F32),
        V((2, end1, 128), F32), V((end2, 128), F32), V((half_rows, 128), F32), V((n_slab * slab2, 128), F32),
        V((3, PLANE, max(share), 128), F32), V((CUBE, rows2, 128), F32), V((3, SIDE, max(share), 128), F32), V((2, end1, 128), F32), V((end2, 128), F32),
        D((7,)), *link_sems, D((2,)), D((2,)), D((1,)), D((3,)), D((2,)), D, D((3,)), D((5,)), D((7,)), D, D, D, pltpu.SemaphoreType.REGULAR((2,)),
    ]
    out_bytes = 4 * (slab1 * hid + slab2 * hid + slab1 * nodes)
    any_spec = pl.BlockSpec(memory_space=pl.ANY)
    vmem_spec = pl.BlockSpec(memory_space=pltpu.VMEM)
    return pl.pallas_call(
        kernel,
        out_shape=(pltpu.VMEM((feat, hid), F32), pltpu.VMEM((cls, hid), F32), pltpu.VMEM((feat, nodes), F32)),
        in_specs=[any_spec] * 7,
        out_specs=(vmem_spec, vmem_spec, vmem_spec),
        scratch_shapes=scratch,
        compiler_params=pltpu.CompilerParams(collective_id=0, has_side_effects=True, vmem_limit_bytes=VMEM_BYTES - out_bytes - 65536),
        name="gcn_backward",
    )


def write_out(feat, hid, cls, nodes):
    def kernel(dw1, dw2, gf, dw1_out, dw2_out, gf_out, sems):
        pairs = [(dw1, dw1_out), (dw2, dw2_out)]
        for i in range(WRITES):
            cols = pl.ds(i * (nodes // WRITES), nodes // WRITES)
            pairs.append((gf.at[:, cols], gf_out.at[:, cols]))
        copies = [pltpu.make_async_copy(a, b, sems.at[i]) for i, (a, b) in enumerate(pairs)]
        for cp in copies:
            cp.start()
        for cp in copies:
            cp.wait()

    return pl.pallas_call(
        kernel,
        out_shape=(jax.ShapeDtypeStruct((feat, hid), F32), jax.ShapeDtypeStruct((cls, hid), F32), jax.ShapeDtypeStruct((feat, nodes), F32)),
        in_specs=[pl.BlockSpec(memory_space=pltpu.VMEM)] * 3,
        out_specs=(pl.BlockSpec(memory_space=pl.ANY),) * 3,
        scratch_shapes=[pltpu.SemaphoreType.DMA((2 + WRITES,))],
        compiler_params=pltpu.CompilerParams(vmem_limit_bytes=4 * 1024 * 1024),
        name="write_out",
    )


def solution(mesh):
    axis_size = mesh.shape["nodes"]
    row_spec = P(("graph", "nodes"), None)
    replicated = P(None, None)
    part_spec = P("graph", None)

    def device_step(node_feats, a_int, a_halo, send_idx, w_first, w_second, grad_out):
        nodes, feat = node_feats.shape
        hid, cls = w_second.shape
        call = build(axis_size, nodes, feat, hid, cls, send_idx.shape[1])
        dw1, dw2, gf = call(node_feats.T, a_int, a_halo, send_idx, w_first, w_second.T, grad_out.T)
        dw1, dw2, gf = write_out(feat, hid, cls, nodes)(dw1, dw2, gf)
        return dw1, dw2.T, gf.T

    return jax.shard_map(device_step, mesh=mesh, in_specs=(row_spec, row_spec, row_spec, row_spec, replicated, replicated, row_spec), out_specs=(part_spec, part_spec, row_spec), check_vma=False)
```

```python
import jax
import jax.numpy as jnp
from jax import lax
from jax.experimental import pallas as pl
from jax.experimental.pallas import tpu as pltpu
from jax.sharding import PartitionSpec as P

F32 = jnp.float32
BF16 = jnp.bfloat16
SIDE = 4
PLANE = SIDE * SIDE
CUBE = PLANE * SIDE
OFFSETS = (1, -1, 2, -2)
LINKS = 4
VMEM_BYTES = 67043328
WRITES = 1


def dot(a, b, ca, cb):
    return lax.dot_general(a, b, (((ca,), (cb,)), ((), ())), preferred_element_type=F32)


def hops(step):
    return sum(min(d, SIDE - d) for d in step)


PLANE_PEERS = sorted(((a, b) for a in range(SIDE) for b in range(SIDE) if a or b), key=hops, reverse=True)
CUBE_PEERS = sorted(((a, b, c) for a in range(SIDE) for b in range(SIDE) for c in range(SIDE) if a or b or c), key=hops, reverse=True)


RELEASE = ((0.0, 0.5, 0.9, 1.1), (0.0, 0.6, 1.2, 1.4), (0.0, 0.9, 1.8, 2.4))


def release_order(dims):
    spots = [()]
    for _ in dims:
        spots = [s + (c,) for s in spots for c in range(SIDE)]
    return sorted(spots, key=lambda s: sum(RELEASE[d][c] for d, c in zip(dims, s)))


class Piece:
    def __init__(self, num, plane, cross, rows, base):
        self.num, self.plane, self.cross, self.rows, self.base = num, plane, cross, rows, base

    def steps(self, ab):
        st = [0, 0, 0]
        st[self.plane[0]], st[self.plane[1]] = ab
        return tuple(st)

    def across(self, step):
        st = [0, 0, 0]
        st[self.cross] = step
        return tuple(st)


def build(n_dev, nodes, feat, hid, cls, slots):
    all_slots = LINKS * slots
    half_hid = hid // 2
    n_slab = hid // 128
    slab1 = (feat + 7) // 8 * 8
    slab2 = (cls + 7) // 8 * 8
    half_rows = n_slab // 2 * slab1
    units = -(-half_rows // (PLANE * 8))
    share = [8 * ((units + 2 - p) // 3) for p in range(3)]
    pieces, end1 = [], 0
    for num, (dims, rows) in enumerate(zip((((1, 2), 0), ((0, 1), 2), ((0, 2), 1)), share)):
        pieces.append(Piece(num, dims[0], dims[1], rows, end1))
        end1 += rows * PLANE
    rows1 = sum(share)
    rows2 = -(-n_slab * slab2 // (CUBE * 8)) * 8
    end2 = rows2 * CUBE

    def kernel(h0_hbm, aint_hbm, ahalo_hbm, idx_hbm, w0_hbm, w1_hbm, g_hbm,
               dw1_out, dw2_out, gf_out,
               h0, aint, ahalo, idx, w0, w1, g,
               pt, e1, z0, ft, e0,
               s0, halo0, o1, r1, sz, haloz, o0, r0,
               z0acc, d1acc, z1acc, gfacc,
               part1, part2, pair1_in, pair2_in, rs1_in, rs2_in, x_in, res1, res2,
               in_sem, fwd_sem, bwd_sem, zcp_sem, ocp_sem,
               pair1_sem, pair2_sem, rs1_sem, rs1_r, rs2_sem, x_s, x_r, ag1_r, ag2_r, back1_s, back2_s, early_s, gossip):
        me = lax.axis_index("nodes")
        core = lax.rem(me, 2)
        coord = (lax.rem(me // 2, SIDE), lax.rem(me // (2 * SIDE), SIDE), me // (2 * SIDE * SIDE))
        stride = (2, 2 * SIDE, 2 * SIDE * SIDE)
        mate = me + 1 - 2 * core

        def ring_steps(dim, c):
            d = lax.rem(coord[dim] + (SIDE - c), SIDE)
            return d * (SIDE - d) - d * (SIDE - d) // 3 * 2

        away = [[ring_steps(dim, c) for c in range(SIDE)] for dim in range(3)]

        def moved(dim, step):
            return lax.rem(coord[dim] + step, SIDE)

        def peer(steps):
            d = core
            for dim in range(3):
                d = d + moved(dim, steps[dim]) * stride[dim]
            return d

        def near(o):
            return lax.rem(me + (o + n_dev), n_dev)

        def signal(sem, d):
            pl.semaphore_signal(sem, inc=1, device_id={"nodes": d}, device_id_type=pl.DeviceIdType.MESH)

        def rcopy(src, dst, ss, rs, d):
            return pltpu.make_async_remote_copy(src_ref=src, dst_ref=dst, send_sem=ss, recv_sem=rs,
                                                device_id={"nodes": d}, device_id_type=pl.DeviceIdType.MESH)

        def lanes(ref, k):
            return ref.at[:, pl.ds(k * slots, slots)]

        def link_copies(src, dst, sems, sign):
            return [rcopy(lanes(src, k), lanes(dst, k), sems.at[0], sems.at[1 + k // 2], near(sign * OFFSETS[k])) for k in range(LINKS)]

        def link_wait(src, dst, sems, i):
            both = pl.ds(2 * i * slots, 2 * slots)
            rcopy(src.at[:, both], dst.at[:, both], sems.at[0], sems.at[1 + i], mate).wait_recv()

        def links_sent():
            for src, dst, sems in ((s0, halo0, fwd_sem), (o1, r1, bwd_sem), (sz, haloz, zcp_sem), (o0, r0, ocp_sem)):
                rcopy(src, dst, sems.at[0], sems.at[1], mate).wait_send()

        def start(copies):
            for cp in copies:
                cp.start()

        def wait(copies):
            for cp in copies:
                cp.wait()

        def on(which, name, *steps):
            @pl.when(core == which)
            def _():
                with jax.named_scope(name):
                    for step in steps:
                        step()

        barrier = pltpu.get_barrier_semaphore()
        ring = [peer(tuple(step if d == dim else 0 for d in range(3))) for dim in range(3) for step in (1, SIDE - 1)]
        greeted = [near(o) for o in OFFSETS] + [mate] + ring
        for d in greeted:
            signal(barrier, d)

        loads = [pltpu.make_async_copy(a, b, in_sem.at[i]) for i, (a, b) in enumerate((
            (idx_hbm, idx), (h0_hbm, h0), (g_hbm, g), (w1_hbm, w1), (ahalo_hbm, ahalo), (aint_hbm, aint), (w0_hbm, w0)))]
        start(loads)
        ld_idx, ld_h0, ld_g, ld_w1, ld_ahalo, ld_aint, ld_w0 = loads

        def gossip_send(i):
            for d in ring:
                signal(gossip.at[i % 2], d)

        def gossip_wait(i):
            pl.semaphore_wait(gossip.at[i % 2], len(ring))

        part1[...] = jnp.zeros_like(part1)
        part2[...] = jnp.zeros_like(part2)
        node_id = lax.broadcasted_iota(jnp.int32, (nodes, slots), 0)
        fwd = link_copies(s0, halo0, fwd_sem, 1)
        bwd = link_copies(o1, r1, bwd_sem, -1)
        zcp = link_copies(sz, haloz, zcp_sem, 1)
        ocp = link_copies(o0, r0, ocp_sem, -1)
        upper = pl.ds(2 * slots, 2 * slots)
        lower = pl.ds(0, 2 * slots)

        def select_rows(ks):
            for k in ks:
                pt[:, k * slots:(k + 1) * slots] = jnp.where(node_id == idx[k:k + 1, :], 1.0, 0.0).astype(BF16)

        with jax.named_scope("ld_idx"):
            ld_idx.wait()
        with jax.named_scope("pt"):
            select_rows((2, 3))
        with jax.named_scope("ld_h0"):
            ld_h0.wait()
        with jax.named_scope("s0"):
            s0[:, upper] = dot(h0[...], pt[:, upper], 1, 0).astype(BF16)
        with jax.named_scope("s0_low"):
            select_rows((0, 1))
            s0[:, lower] = dot(h0[...], pt[:, lower], 1, 0).astype(BF16)
        with jax.named_scope("barrier"):
            pl.semaphore_wait(barrier, len(greeted))
        with jax.named_scope("fwd_start"):
            start(fwd[2:] + fwd[:2])
            gossip_send(0)
        with jax.named_scope("e1"):
            ld_g.wait()
            ld_w1.wait()
            e1[...] = dot(w1[...], g[...], 0, 0).astype(BF16)
        with jax.named_scope("o1"):
            ld_ahalo.wait()
            o1[...] = dot(e1[...], ahalo[...], 1, 0).astype(BF16)
        on(0, "bwd_start0", lambda: start([bwd[2], bwd[0], bwd[1]]))
        on(1, "bwd_start1", lambda: start([bwd[3], bwd[1], bwd[0]]))
        with jax.named_scope("z0acc"):
            ld_aint.wait()
            z0acc[...] = dot(h0[...], aint[...], 1, 1)
        on(0, "bwd_rest0", bwd[3].start)
        on(1, "bwd_rest1", bwd[2].start)
        with jax.named_scope("gossip0"):
            gossip_wait(0)
            gossip_send(1)
        with jax.named_scope("d1acc"):
            d1acc[...] = dot(e1[...], aint[...], 1, 0)

        with jax.named_scope("fwd_wait_up"):
            link_wait(s0, halo0, fwd_sem, 1)
        with jax.named_scope("z0_up"):
            z0acc[...] = z0acc[...] + dot(halo0[:, upper], ahalo[:, upper], 1, 1)
        with jax.named_scope("fwd_wait_low"):
            link_wait(s0, halo0, fwd_sem, 0)
        with jax.named_scope("z0"):
            z0[...] = (z0acc[...] + dot(halo0[:, lower], ahalo[:, lower], 1, 1)).astype(BF16)
        halves = (zcp[:2], zcp[2:])
        for n in range(2):
            with jax.named_scope("sz%d" % n):
                cols = pl.ds(pl.multiple_of((core if n else 1 - core) * 2 * slots, 2 * slots), 2 * slots)
                sz[:, cols] = dot(z0[...], pt[:, cols], 1, 0).astype(BF16)
            on(0, "z_start%d" % n, lambda: start(halves[1 - n]))
            on(1, "z_start%d" % n, lambda: start(halves[n]))
        with jax.named_scope("gossip1"):
            gossip_wait(1)
            gossip_send(2)
        with jax.named_scope("h1"):
            ld_w0.wait()
            ft[...] = jnp.maximum(dot(w0[...], z0[...], 0, 0), 0.0).astype(BF16)
        with jax.named_scope("z1acc"):
            z1acc[...] = dot(ft[...], aint[...], 1, 1)
        with jax.named_scope("gossip2"):
            gossip_wait(2)
            gossip_send(3)

        with jax.named_scope("bwd_wait_up"):
            link_wait(o1, r1, bwd_sem, 1)
        with jax.named_scope("d1_up"):
            d1acc[...] = d1acc[...] + dot(r1[:, upper], pt[:, upper], 1, 1)
        with jax.named_scope("bwd_wait_low"):
            link_wait(o1, r1, bwd_sem, 0)

        def first_half(h):
            rows = pl.ds(pl.multiple_of(h * half_hid, half_hid), half_hid)
            d1 = d1acc[rows, :] + dot(r1[rows, lower], pt[:, lower], 1, 1)
            ft[rows, :] = jnp.where(ft[rows, :] > 0, d1, 0.0).astype(BF16)
            dw1 = dot(z0[...], ft[rows, :], 1, 1)
            for s in range(half_hid // 128):
                part1[h, pl.ds(s * slab1, feat), :] = dw1[:, s * 128:(s + 1) * 128]

        def rows_of(ref, n, i):
            return ref.at[pl.ds(pl.multiple_of(i * n, 8), n), :]

        def rows_wait(ref, rows, ss, rs):
            some = ref.at[pl.ds(0, rows), :]
            if ss is not None:
                rcopy(some, some, ss, ss, mate).wait_send()
            if rs is not None:
                rcopy(some, some, rs, rs, mate).wait_recv()

        pair1 = rcopy(part1.at[1 - core, pl.ds(0, half_rows), :], pair1_in, pair1_sem.at[0], pair1_sem.at[1], mate)

        def plane_id(p, ab=(0, 0)):
            return moved(p.plane[0], ab[0]) * SIDE + moved(p.plane[1], ab[1])

        def chunk1(ref, p, i):
            return ref.at[core, pl.ds(pl.multiple_of(p.base + i * p.rows, 8), p.rows), :]

        def stage(ref, p, i):
            return ref.at[p.num, i, pl.ds(0, p.rows), :]

        def rs1_send(group):
            start([rcopy(chunk1(part1, p, plane_id(p, ab)), stage(rs1_in, p, plane_id(p)), rs1_sem.at[0], rs1_r.at[p.num], peer(p.steps(ab)))
                   for ab in PLANE_PEERS for p in group])
            for p in group:
                rs1_in[p.num, plane_id(p), pl.ds(0, p.rows), :] = part1[core, pl.ds(pl.multiple_of(p.base + plane_id(p) * p.rows, 8), p.rows), :]

        def rs1_start():
            used = pl.ds(0, half_rows)
            part1[core, used, :] = part1[core, used, :] + pair1_in[...]
            rs1_send(pieces)

        def rs1_finish():
            for p in pieces:
                rows_wait(part1.at[0], (PLANE - 1) * p.rows, None, rs1_r.at[p.num])
                total = rs1_in[p.num, 0, 0:p.rows, :]
                for i in range(1, PLANE):
                    total = total + rs1_in[p.num, i, 0:p.rows, :]
                mine = stage(x_in, p, coord[p.cross])
                x_in[p.num, coord[p.cross], pl.ds(0, p.rows), :] = total
                start([rcopy(mine, mine, x_s, x_r.at[p.num], peer(p.across(step))) for step in (2, 1, 3)])
            rows_wait(part1.at[0], (PLANE - 1) * rows1, rs1_sem.at[0], None)

        def x1_finish():
            for p in pieces:
                rows_wait(part1.at[0], (SIDE - 1) * p.rows, None, x_r.at[p.num])
                total = x_in[p.num, 0, 0:p.rows, :]
                for i in range(1, SIDE):
                    total = total + x_in[p.num, i, 0:p.rows, :]
                res1[core, pl.ds(pl.multiple_of(p.base + plane_id(p) * p.rows, 8), p.rows), :] = total
                mine = chunk1(res1, p, plane_id(p))
                for a, b in release_order(p.plane):
                    steps = away[p.plane[0]][a] + away[p.plane[1]][b]
                    d = core + a * stride[p.plane[0]] + b * stride[p.plane[1]] + coord[p.cross] * stride[p.cross]
                    rcopy(mine, mine, rs1_sem.at[0], ag1_r.at[steps], d + jnp.where(steps == 0, mate - me, 0)).start()
            rows_wait(part1.at[0], (SIDE - 1) * rows1, x_s, None)

        def back1(p, i):
            return rcopy(chunk1(res1, p, i), chunk1(res1, p, i), back1_s, ag1_r.at[0], mate)

        def ag1_step(n):
            near_n = [ab for ab in PLANE_PEERS if hops(ab) == n]
            rows_wait(part1.at[0], len(near_n) * rows1, None, ag1_r.at[n])
            start([back1(p, plane_id(p, ab)) for ab in near_n for p in pieces])

        def back1_finish():
            rows_wait(part1.at[0], PLANE * rows1, None, ag1_r.at[0])

        def back1_sent():
            rows_wait(part1.at[0], PLANE * rows1, rs1_sem.at[0], None)
            rows_wait(part1.at[0], (PLANE - 1) * rows1, back1_s, None)

        my_cube = coord[0] + SIDE * (coord[1] + SIDE * coord[2])
        pair2 = rcopy(part2.at[pl.ds(0, n_slab * slab2), :], pair2_in, pair2_sem.at[0], pair2_sem.at[1], mate)

        def cube_id(steps):
            return moved(0, steps[0]) + SIDE * (moved(1, steps[1]) + SIDE * moved(2, steps[2]))

        def rs2_start():
            pair2.wait_recv()
            used = pl.ds(0, n_slab * slab2)
            part2[used, :] = part2[used, :] + pair2_in[...]
            start([rcopy(rows_of(part2, rows2, cube_id(st)), rs2_in.at[my_cube], rs2_sem.at[0], rs2_sem.at[1], peer(st)) for st in CUBE_PEERS])
            rs2_in[my_cube] = part2[pl.ds(pl.multiple_of(my_cube * rows2, 8), rows2), :]

        def rs2_finish():
            rows_wait(part2, (CUBE - 1) * rows2, rs2_sem.at[0], rs2_sem.at[1])
            sums = [rs2_in[i] for i in range(CUBE)]
            while len(sums) > 1:
                sums = [a + b for a, b in zip(sums[::2], sums[1::2])]
            res2[pl.ds(pl.multiple_of(my_cube * rows2, 8), rows2), :] = sums[0]
            mine = rows_of(res2, rows2, my_cube)
            for a, b, c in release_order((0, 1, 2)):
                steps = away[0][a] + away[1][b] + away[2][c]
                d = core + a * stride[0] + b * stride[1] + c * stride[2]
                rcopy(mine, mine, rs2_sem.at[0], ag2_r.at[steps], d + jnp.where(steps == 0, mate - me, 0)).start()
                if (a, b, c) == (0, 0, 0):
                    pl.when(me != 1)(rcopy(mine, mine, early_s, ag2_r.at[0], 0).start)

        def back2(i):
            return rcopy(rows_of(res2, rows2, i), rows_of(res2, rows2, i), back2_s, ag2_r.at[0], mate)

        def ag2_step(n):
            near_n = [st for st in CUBE_PEERS if hops(st) == n]
            rows_wait(part2, len(near_n) * rows2, None, ag2_r.at[n])
            pl.when(me != 1)(lambda: start([back2(cube_id(st)) for st in near_n]))

        def ag2_finish():
            rows_wait(part2, CUBE * rows2, rs2_sem.at[0], None)

            @pl.when(me != 1)
            def _():
                rows_wait(part2, (CUBE - 1) * rows2, back2_s, None)
                rows_wait(part2, rows2, early_s, None)

        def run(name, *steps):
            with jax.named_scope(name):
                for step in steps:
                    step()

        run("half_mate", lambda: first_half(1 - core))
        run("pair1_start", pair1.start)
        run("half_own", lambda: first_half(core))
        with jax.named_scope("e0"):
            e0[...] = dot(w0[...], ft[...], 1, 0).astype(BF16)
        with jax.named_scope("gossip3"):
            gossip_wait(3)
            gossip_send(4)
        run("pair1_wait", pair1.wait)
        run("rs1_start", rs1_start)

        def z1_half(n):
            cols = pl.ds(pl.multiple_of((core if n else 1 - core) * 2 * slots, 2 * slots), 2 * slots)
            on(0, "z_wait%d" % n, lambda: link_wait(sz, haloz, zcp_sem, 1 - n))
            on(1, "z_wait%d" % n, lambda: link_wait(sz, haloz, zcp_sem, n))
            with jax.named_scope("z1_%d" % n):
                h1h = jnp.maximum(dot(w0[...], haloz[:, cols], 0, 0), 0.0).astype(BF16)
                return z1acc[...] + dot(h1h, ahalo[:, cols], 1, 1)

        z1acc[...] = z1_half(0)
        z1 = z1_half(1).astype(BF16)
        with jax.named_scope("dw2"):
            dw2 = dot(g[...], z1, 1, 1)
            for s in range(n_slab):
                part2[pl.ds(s * slab2, cls), :] = dw2[:, s * 128:(s + 1) * 128]
        on(0, "pair2_start", pair2.start)
        with jax.named_scope("gossip4"):
            gossip_wait(4)
        with jax.named_scope("o0"):
            o0[...] = dot(e0[...], ahalo[...], 1, 0).astype(BF16)
            pl.when(me == n_dev - 1)(ocp[3].start)
        with jax.named_scope("gfacc"):
            gfacc[...] = dot(e0[...], aint[...], 1, 0)
        on(1, "rs2_start", rs2_start)
        run("rs1_finish", rs1_finish)
        with jax.named_scope("o_start"):
            start(ocp[:3])
            pl.when(me < n_dev - 1)(ocp[3].start)
        run("x1_finish", x1_finish)
        on(1, "rs2_finish", rs2_finish)
        with jax.named_scope("o_wait"):
            link_wait(o0, r0, ocp_sem, 0)
            link_wait(o0, r0, ocp_sem, 1)
        with jax.named_scope("gf"):
            gf_out[...] = gfacc[...] + dot(r0[...], pt[...], 1, 1)
        for n in range(1, 5):
            run("ag1_%d" % n, lambda: ag1_step(n))
        for n in range(1, 7):
            on(1, "ag2_%d" % n, lambda: ag2_step(n))
        run("back1_finish", back1_finish)
        on(0, "back2_wait", lambda: rows_wait(part2, CUBE * rows2, None, ag2_r.at[0]), pair2.wait_send)
        with jax.named_scope("outs"):
            for s in range(n_slab):
                h, q = s // (n_slab // 2), s % (n_slab // 2)
                dw1_out[:, s * 128:(s + 1) * 128] = res1[h, pl.ds(q * slab1, feat), :]
                dw2_out[:, s * 128:(s + 1) * 128] = res2[pl.ds(s * slab2, cls), :]

        run("links_sent", links_sent)
        run("back1_sent", back1_sent)
        on(1, "ag2_finish", ag2_finish)

    V = pltpu.VMEM
    D = pltpu.SemaphoreType.DMA
    link_sems = [D((3,))] * 4
    scratch = [
        V((feat, nodes), BF16), V((nodes, nodes), BF16), V((nodes, all_slots), BF16), V((LINKS, slots), jnp.int32),
        V((feat, hid), BF16), V((cls, hid), BF16), V((cls, nodes), BF16),
        V((nodes, all_slots), BF16), V((hid, nodes), BF16), V((feat, nodes), BF16), V((hid, nodes), BF16), V((feat, nodes), BF16),
        V((feat, all_slots), BF16), V((feat, all_slots), BF16), V((hid, all_slots), BF16), V((hid, all_slots), BF16),
        V((feat, all_slots), BF16), V((feat, all_slots), BF16), V((feat, all_slots), BF16), V((feat, all_slots), BF16),
        V((feat, nodes), F32), V((hid, nodes), F32), V((hid, nodes), F32), V((feat, nodes), F32),
        V((2, end1, 128), F32), V((end2, 128), F32), V((half_rows, 128), F32), V((n_slab * slab2, 128), F32),
        V((3, PLANE, max(share), 128), F32), V((CUBE, rows2, 128), F32), V((3, SIDE, max(share), 128), F32), V((2, end1, 128), F32), V((end2, 128), F32),
        D((7,)), *link_sems, D((2,)), D((2,)), D((1,)), D((3,)), D((2,)), D, D((3,)), D((5,)), D((7,)), D, D, D, pltpu.SemaphoreType.REGULAR((2,)),
    ]
    out_bytes = 4 * (slab1 * hid + slab2 * hid + slab1 * nodes)
    any_spec = pl.BlockSpec(memory_space=pl.ANY)
    vmem_spec = pl.BlockSpec(memory_space=pltpu.VMEM)
    return pl.pallas_call(
        kernel,
        out_shape=(pltpu.VMEM((feat, hid), F32), pltpu.VMEM((cls, hid), F32), pltpu.VMEM((feat, nodes), F32)),
        in_specs=[any_spec] * 7,
        out_specs=(vmem_spec, vmem_spec, vmem_spec),
        scratch_shapes=scratch,
        compiler_params=pltpu.CompilerParams(collective_id=0, has_side_effects=True, vmem_limit_bytes=VMEM_BYTES - out_bytes - 65536),
        name="gcn_backward",
    )


def write_out(feat, hid, cls, nodes):
    def kernel(dw1, dw2, gf, dw1_out, dw2_out, gf_out, sems):
        pairs = [(dw1, dw1_out), (dw2, dw2_out)]
        for i in range(WRITES):
            cols = pl.ds(i * (nodes // WRITES), nodes // WRITES)
            pairs.append((gf.at[:, cols], gf_out.at[:, cols]))
        copies = [pltpu.make_async_copy(a, b, sems.at[i]) for i, (a, b) in enumerate(pairs)]
        for cp in copies:
            cp.start()
        for cp in copies:
            cp.wait()

    return pl.pallas_call(
        kernel,
        out_shape=(jax.ShapeDtypeStruct((feat, hid), F32), jax.ShapeDtypeStruct((cls, hid), F32), jax.ShapeDtypeStruct((feat, nodes), F32)),
        in_specs=[pl.BlockSpec(memory_space=pltpu.VMEM)] * 3,
        out_specs=(pl.BlockSpec(memory_space=pl.ANY),) * 3,
        scratch_shapes=[pltpu.SemaphoreType.DMA((2 + WRITES,))],
        compiler_params=pltpu.CompilerParams(vmem_limit_bytes=4 * 1024 * 1024),
        name="write_out",
    )


def solution(mesh):
    axis_size = mesh.shape["nodes"]
    row_spec = P(("graph", "nodes"), None)
    replicated = P(None, None)
    part_spec = P("graph", None)

    def device_step(node_feats, a_int, a_halo, send_idx, w_first, w_second, grad_out):
        nodes, feat = node_feats.shape
        hid, cls = w_second.shape
        call = build(axis_size, nodes, feat, hid, cls, send_idx.shape[1])
        dw1, dw2, gf = call(node_feats.T, a_int, a_halo, send_idx, w_first, w_second.T, grad_out.T)
        dw1, dw2, gf = write_out(feat, hid, cls, nodes)(dw1, dw2, gf)
        return dw1, dw2.T, gf.T

    return jax.shard_map(device_step, mesh=mesh, in_specs=(row_spec, row_spec, row_spec, row_spec, replicated, replicated, row_spec), out_specs=(part_spec, part_spec, row_spec), check_vma=False)
```
